32 devices in a mesh: batch: 1 (over z), col: 4 (over y), row: 8 (over x, core).
Axes of the slice: x: 4, y: 4, z: 1, core: 2. Of those that a mesh axis runs over, the one named last changes fastest.
The devices are a block of a 4x4x8 slice.
Arguments:
- tokens: bfloat16 [512, 4, 1536], P(('batch', 'row', 'col'))
- mod_vec: float32 [5, 1536], replicated
- w_fc1: bfloat16 [1536, 6144], replicated
- w_fc2: bfloat16 [6144, 1536], replicated
- w_final: bfloat16 [1536, 64], replicated
- conv_in: bfloat16 [3, 3, 16, 512], replicated
- norm_attn: float32 [2, 512], replicated
- w_qkv: bfloat16 [512, 1536], replicated
- w_proj: bfloat16 [512, 512], replicated
- norm0_a: float32 [2, 512], replicated
- conv0_a: bfloat16 [3, 3, 512, 512], replicated
- norm0_b: float32 [2, 512], replicated
- conv0_b: bfloat16 [3, 3, 512, 512], replicated
- upconv_0: bfloat16 [3, 3, 512, 512], replicated
- norm1_a: float32 [2, 512], replicated
- conv1_a: bfloat16 [3, 3, 512, 512], replicated
- norm1_b: float32 [2, 512], replicated
- conv1_b: bfloat16 [3, 3, 512, 512], replicated
- upconv_1: bfloat16 [3, 3, 512, 512], replicated
- norm2_a: float32 [2, 512], replicated
- conv2_a: bfloat16 [3, 3, 512, 256], replicated
- norm2_b: float32 [2, 256], replicated
- conv2_b: bfloat16 [3, 3, 256, 256], replicated
- skip_2: bfloat16 [512, 256], replicated
- upconv_2: bfloat16 [3, 3, 256, 256], replicated
- norm3_a: float32 [2, 256], replicated
- conv3_a: bfloat16 [3, 3, 256, 128], replicated
- norm3_b: float32 [2, 128], replicated
- conv3_b: bfloat16 [3, 3, 128, 128], replicated
- skip_3: bfloat16 [256, 128], replicated
- norm_out: float32 [2, 128], replicated
- conv_out: bfloat16 [3, 3, 128, 3], replicated
Outputs:
- output: float32 [8192, 64, 3], P(('batch', 'row'), 'col')
All inputs are finite; a program needn't handle non-finite values.
Results may differ from the reference program's by a relative error of at most 0.02.
Values are sent between devices in bfloat16 or wider.
A program may use at most 768 MiB of HBM per device.

```python
import jax
import jax.numpy as jnp
from jax import lax

D = 1536
LAT_C = 16
LAT_H = 1024
LAT_W = 8
DEC_CH0 = 512
DEC_CH1 = 512
DEC_CH2 = 256
DEC_CH3 = 128
GROUPS = 32

TOK_H = LAT_H // 2
TOK_W = LAT_W // 2


def draw_weight(rand_key, arr_shape, fan_in):
    return (jax.random.normal(rand_key, arr_shape, jnp.float32) * fan_in ** -0.5).astype(jnp.bfloat16)


def draw_norm(rand_key, num_ch):
    raw_draw = jax.random.normal(rand_key, (2, num_ch), jnp.float32)
    return jnp.stack([1.0 + 0.3 * raw_draw[0], 0.3 * raw_draw[1]])


def setup_inputs(seed: int = 0, part: int = 0) -> dict:
    base_key = jax.random.key(seed)
    part_key = jax.random.fold_in(base_key, part)
    noise_key, dir_key = jax.random.split(part_key, 2)
    row_ramp = (jnp.arange(TOK_H, dtype=jnp.float32) + 0.5) * (2.0 / TOK_H) - 1.0
    col_ramp = (jnp.arange(TOK_W, dtype=jnp.float32) + 0.5) * (2.0 / TOK_W) - 1.0
    directions = jax.random.normal(dir_key, (2, D), jnp.float32)
    tok_noise = jax.random.normal(noise_key, (TOK_H, TOK_W, D), jnp.float32)
    tokens = (tok_noise * (1.0 + 0.6 * row_ramp[:, None, None])
              + 1.5 * row_ramp[:, None, None] * directions[0]
              + 1.2 * col_ramp[None, :, None] * directions[1])
    weight_keys = jax.random.split(base_key, 31)
    gate_shift = jnp.array([0.0, 0.0, 1.0, 0.0, 0.0], jnp.float32)
    mod_vec = 0.5 * jax.random.normal(weight_keys[0], (5, D), jnp.float32) + gate_shift[:, None]
    inputs = dict(
        tokens=tokens.astype(jnp.bfloat16),
        mod_vec=mod_vec,
        w_fc1=draw_weight(weight_keys[1], (D, 4 * D), D),
        w_fc2=draw_weight(weight_keys[2], (4 * D, D), 4 * D),
        w_final=draw_weight(weight_keys[3], (D, 4 * LAT_C), D),
        conv_in=draw_weight(weight_keys[4], (3, 3, LAT_C, DEC_CH0), 9 * LAT_C),
        norm_attn=draw_norm(weight_keys[5], DEC_CH0),
        w_qkv=draw_weight(weight_keys[6], (DEC_CH0, 3 * DEC_CH0), DEC_CH0),
        w_proj=draw_weight(weight_keys[7], (DEC_CH0, DEC_CH0), DEC_CH0),
        norm0_a=draw_norm(weight_keys[8], DEC_CH0),
        conv0_a=draw_weight(weight_keys[9], (3, 3, DEC_CH0, DEC_CH0), 9 * DEC_CH0),
        norm0_b=draw_norm(weight_keys[10], DEC_CH0),
        conv0_b=draw_weight(weight_keys[11], (3, 3, DEC_CH0, DEC_CH0), 9 * DEC_CH0),
        upconv_0=draw_weight(weight_keys[12], (3, 3, DEC_CH0, DEC_CH0), 9 * DEC_CH0),
        norm1_a=draw_norm(weight_keys[13], DEC_CH0),
        conv1_a=draw_weight(weight_keys[14], (3, 3, DEC_CH0, DEC_CH1), 9 * DEC_CH0),
        norm1_b=draw_norm(weight_keys[15], DEC_CH1),
        conv1_b=draw_weight(weight_keys[16], (3, 3, DEC_CH1, DEC_CH1), 9 * DEC_CH1),
        upconv_1=draw_weight(weight_keys[17], (3, 3, DEC_CH1, DEC_CH1), 9 * DEC_CH1),
        norm2_a=draw_norm(weight_keys[18], DEC_CH1),
        conv2_a=draw_weight(weight_keys[19], (3, 3, DEC_CH1, DEC_CH2), 9 * DEC_CH1),
        norm2_b=draw_norm(weight_keys[20], DEC_CH2),
        conv2_b=draw_weight(weight_keys[21], (3, 3, DEC_CH2, DEC_CH2), 9 * DEC_CH2),
        skip_2=draw_weight(weight_keys[22], (DEC_CH1, DEC_CH2), DEC_CH1),
        upconv_2=draw_weight(weight_keys[23], (3, 3, DEC_CH2, DEC_CH2), 9 * DEC_CH2),
        norm3_a=draw_norm(weight_keys[24], DEC_CH2),
        conv3_a=draw_weight(weight_keys[25], (3, 3, DEC_CH2, DEC_CH3), 9 * DEC_CH2),
        norm3_b=draw_norm(weight_keys[26], DEC_CH3),
        conv3_b=draw_weight(weight_keys[27], (3, 3, DEC_CH3, DEC_CH3), 9 * DEC_CH3),
        skip_3=draw_weight(weight_keys[28], (DEC_CH2, DEC_CH3), DEC_CH2),
        norm_out=draw_norm(weight_keys[29], DEC_CH3),
        conv_out=draw_weight(weight_keys[30], (3, 3, DEC_CH3, 3), 9 * DEC_CH3),
    )
    return inputs


def layer_norm(tok_vals):
    tok_mean = jnp.mean(tok_vals, axis=-1, keepdims=True)
    tok_var = jnp.mean(jnp.square(tok_vals - tok_mean), axis=-1, keepdims=True)
    return (tok_vals - tok_mean) * lax.rsqrt(tok_var + 1e-6)


def group_norm(feat_map, norm_par, use_silu):
    img_h, img_w, num_ch = feat_map.shape
    grouped = feat_map.astype(jnp.float32).reshape(img_h, img_w, GROUPS, num_ch // GROUPS)
    pix_count = img_h * img_w * (num_ch // GROUPS)
    grp_mean = jnp.sum(grouped, axis=(0, 1, 3)) / pix_count
    grp_var = jnp.sum(jnp.square(grouped), axis=(0, 1, 3)) / pix_count - jnp.square(grp_mean)
    normed = (grouped - grp_mean[:, None]) * lax.rsqrt(grp_var + 1e-6)[:, None]
    normed = normed.reshape(img_h, img_w, num_ch) * norm_par[0] + norm_par[1]
    if use_silu:
        normed = jax.nn.silu(normed)
    return normed.astype(jnp.bfloat16)


def conv_same(feat_map, kernel):
    summed = lax.conv_general_dilated(feat_map.astype(jnp.float32)[None], kernel.astype(jnp.float32), (1, 1), ((1, 1), (1, 1)), dimension_numbers=('NHWC', 'HWIO', 'NHWC'), preferred_element_type=jnp.float32)
    return summed[0]


def upsample_two(feat_map):
    img_h, img_w, num_ch = feat_map.shape
    wide_map = jnp.broadcast_to(feat_map[:, None, :, None, :], (img_h, 2, img_w, 2, num_ch))
    return wide_map.reshape(2 * img_h, 2 * img_w, num_ch)


def res_block(feat_map, norm_a, conv_a, norm_b, conv_b, skip_w):
    hidden = conv_same(group_norm(feat_map, norm_a, True), conv_a).astype(jnp.bfloat16)
    branch = conv_same(group_norm(hidden, norm_b, True), conv_b)
    img_h, img_w, num_ch = feat_map.shape
    if skip_w is None:
        shortcut = feat_map.astype(jnp.float32)
    else:
        shortcut = jnp.dot(feat_map.reshape(img_h * img_w, num_ch), skip_w, preferred_element_type=jnp.float32).reshape(img_h, img_w, skip_w.shape[1])
    return (shortcut + branch).astype(jnp.bfloat16)


def mid_attention(feat_map, norm_par, w_qkv, w_proj):
    img_h, img_w, num_ch = feat_map.shape
    normed = group_norm(feat_map, norm_par, False).reshape(img_h * img_w, num_ch)
    qkv_all = jnp.dot(normed, w_qkv, preferred_element_type=jnp.float32).astype(jnp.bfloat16)
    queries = qkv_all[:, :num_ch].reshape(img_h, img_w, num_ch)
    keys_all = qkv_all[:, num_ch:2 * num_ch].astype(jnp.float32)
    values_all = qkv_all[:, 2 * num_ch:].astype(jnp.float32)

    def row_attend(query_row):
        scores = jnp.dot(query_row.astype(jnp.float32), keys_all.T) * num_ch ** -0.5
        attn_probs = jax.nn.softmax(scores, axis=-1).astype(jnp.bfloat16)
        return jnp.dot(attn_probs.astype(jnp.float32), values_all).astype(jnp.bfloat16)

    attended = lax.map(row_attend, queries).reshape(img_h * img_w, num_ch)
    summed = feat_map.reshape(img_h * img_w, num_ch).astype(jnp.float32) + jnp.dot(attended, w_proj, preferred_element_type=jnp.float32)
    return summed.astype(jnp.bfloat16).reshape(img_h, img_w, num_ch)


def decode(latent, params):
    feat_map = conv_same(latent, params['conv_in']).astype(jnp.bfloat16)
    feat_map = mid_attention(feat_map, params['norm_attn'], params['w_qkv'], params['w_proj'])
    feat_map = res_block(feat_map, params['norm0_a'], params['conv0_a'], params['norm0_b'], params['conv0_b'], None)
    feat_map = conv_same(upsample_two(feat_map), params['upconv_0']).astype(jnp.bfloat16)
    feat_map = res_block(feat_map, params['norm1_a'], params['conv1_a'], params['norm1_b'], params['conv1_b'], None)
    feat_map = conv_same(upsample_two(feat_map), params['upconv_1']).astype(jnp.bfloat16)
    feat_map = res_block(feat_map, params['norm2_a'], params['conv2_a'], params['norm2_b'], params['conv2_b'], params['skip_2'])
    feat_map = conv_same(upsample_two(feat_map), params['upconv_2']).astype(jnp.bfloat16)
    feat_map = res_block(feat_map, params['norm3_a'], params['conv3_a'], params['norm3_b'], params['conv3_b'], params['skip_3'])
    return conv_same(group_norm(feat_map, params['norm_out'], True), params['conv_out'])


def reference(tokens, mod_vec, w_fc1, w_fc2, w_final, conv_in, norm_attn, w_qkv, w_proj, norm0_a, conv0_a, norm0_b, conv0_b, upconv_0, norm1_a, conv1_a, norm1_b, conv1_b, upconv_1, norm2_a, conv2_a, norm2_b, conv2_b, skip_2, upconv_2, norm3_a, conv3_a, norm3_b, conv3_b, skip_3, norm_out, conv_out):
    tok_f = tokens.reshape(TOK_H * TOK_W, D).astype(jnp.float32)
    act_in = (layer_norm(tok_f) * (1.0 + mod_vec[1]) + mod_vec[0]).astype(jnp.bfloat16)
    hidden = jax.nn.gelu(jnp.dot(act_in, w_fc1, preferred_element_type=jnp.float32), approximate=True).astype(jnp.bfloat16)
    resid_tok = (tok_f + mod_vec[2] * jnp.dot(hidden, w_fc2, preferred_element_type=jnp.float32)).astype(jnp.bfloat16)
    final_in = (layer_norm(resid_tok.astype(jnp.float32)) * (1.0 + mod_vec[4]) + mod_vec[3]).astype(jnp.bfloat16)
    patch_out = jnp.dot(final_in, w_final, preferred_element_type=jnp.float32).astype(jnp.bfloat16)
    latent = patch_out.reshape(TOK_H, TOK_W, 2, 2, LAT_C).transpose(0, 2, 1, 3, 4).reshape(LAT_H, LAT_W, LAT_C)
    params = dict(conv_in=conv_in, norm_attn=norm_attn, w_qkv=w_qkv, w_proj=w_proj, norm0_a=norm0_a, conv0_a=conv0_a, norm0_b=norm0_b, conv0_b=conv0_b, upconv_0=upconv_0, norm1_a=norm1_a, conv1_a=conv1_a, norm1_b=norm1_b, conv1_b=conv1_b, upconv_1=upconv_1, norm2_a=norm2_a, conv2_a=conv2_a, norm2_b=norm2_b, conv2_b=conv2_b, skip_2=skip_2, upconv_2=upconv_2, norm3_a=norm3_a, conv3_a=conv3_a, norm3_b=norm3_b, conv3_b=conv3_b, skip_3=skip_3, norm_out=norm_out, conv_out=conv_out)
    return decode(latent, params)
```

```python
import functools
import jax
import jax.numpy as jnp
from jax import lax
from jax.experimental import pallas as pl
from jax.experimental.pallas import tpu as pltpu
from jax.sharding import PartitionSpec as P

GROUPS = 32
LANES = 128
F32, BF16 = jnp.float32, jnp.bfloat16
MESH = pl.DeviceIdType.MESH
VMEM_SPEC = pl.BlockSpec(memory_space=pltpu.VMEM)
MIB = 1 << 20
TOTALS = jax.ShapeDtypeStruct((1, LANES), F32)


def dot(a, b):
    return jnp.dot(a, b, preferred_element_type=F32)


def dot_t(a, b):
    return lax.dot_general(a, b, (((1,), (1,)), ((), ())), preferred_element_type=F32)


def exact_dot(a, b):
    return jnp.dot(a, b, preferred_element_type=F32, precision=lax.Precision.HIGHEST)


def clear(*refs):
    for ref in refs:
        ref[...] = jnp.zeros_like(ref)


def iota(shape, dim):
    return lax.broadcasted_iota(jnp.int32, shape, dim)


def aligned(first, size, unit):
    return pl.ds(pl.multiple_of(first, unit), size)


def layer_norm(v):
    mean = jnp.mean(v, axis=-1, keepdims=True)
    var = jnp.mean(jnp.square(v - mean), axis=-1, keepdims=True)
    return (v - mean) * lax.rsqrt(var + 1e-6)


def silu(v):
    half = 0.5 * v
    return half + half * jnp.tanh(half)


class Net:
    def __init__(self, n_row, n_col):
        self.n_col = n_col
        self.n = n_row * n_col
        self.strip = lax.axis_index('row') * n_col + lax.axis_index('col')

    def device(self, ahead):
        other = lax.rem(self.strip + ahead, self.n)
        return {'row': other // self.n_col, 'col': lax.rem(other, self.n_col)}

    def greet(self):
        barrier = pltpu.get_barrier_semaphore()
        for k in range(1, self.n):
            pl.semaphore_signal(barrier, inc=1, device_id=self.device(k), device_id_type=MESH)

    def all_here(self):
        pl.semaphore_wait(pltpu.get_barrier_semaphore(), self.n - 1)

    def to_all(self, src, recv, sems):
        copies = []
        for k in range(1, self.n):
            copy = pltpu.make_async_remote_copy(
                src_ref=src, dst_ref=recv.at[self.strip], send_sem=sems.at[0, k], recv_sem=sems.at[1, k],
                device_id=self.device(k), device_id_type=MESH)
            copy.start()
            copies.append(copy)
        return copies

    def to_sides(self, first, last, hrecv, sems):
        copies = []
        for side, (src, ahead) in enumerate(((last, 1), (first, self.n - 1))):
            copy = pltpu.make_async_remote_copy(
                src_ref=src, dst_ref=hrecv.at[side], send_sem=sems.at[0, side], recv_sem=sems.at[1, side],
                device_id=self.device(ahead), device_id_type=MESH)
            copy.start()
            copies.append(copy)
        return copies


def net_scratch(n, edge_shape=None):
    scratch = [pltpu.VMEM((1, LANES), F32), pltpu.VMEM((n, 1, LANES), F32), pltpu.SemaphoreType.DMA((2, n))]
    if edge_shape is not None:
        scratch += [pltpu.VMEM((2,) + edge_shape, BF16), pltpu.SemaphoreType.DMA((2, 2))]
    return scratch


def exchange(net, stat, stat_ref, recv, sems, tot_ref, sides=None):
    stat_ref[...] = stat
    net.all_here()
    copies = net.to_all(stat_ref, recv, sems)
    if sides is not None:
        first, last, hrecv, hsems, top, bottom = sides
        side_copies = net.to_sides(first, last, hrecv, hsems)
    recv[net.strip] = stat
    for copy in copies:
        copy.wait()
    tot_ref[...] = jnp.sum(recv[...], axis=0)
    if sides is not None:
        for copy, side, dst in zip(side_copies, (0, 1), (top, bottom)):
            copy.wait()
            dst[...] = hrecv[side]


def sum_scratch(ch):
    return [pltpu.VMEM((8, ch), F32)] * 2


def comm_params(cid, mib):
    return pltpu.CompilerParams(collective_id=cid, has_side_effects=True, vmem_limit_bytes=mib * MIB)


def mlp_kernel(net_shape, x_ref, mod_ref, w1_ref, w2_ref, wf_ref, o_ref, a_ref, acc_ref, tok_ref, mix_ref, lat_ref, recv, sems):
    step = pl.program_id(0)
    net = Net(*net_shape)
    shift1, scale1, gate1, shift2, scale2 = [mod_ref[pl.ds(i, 1)] for i in range(5)]

    @pl.when(step == 0)
    def _():
        net.greet()
        v = x_ref[...].astype(F32)
        a_ref[...] = (layer_norm(v) * (1.0 + scale1) + shift1).astype(BF16)
        clear(acc_ref)

    hid = jax.nn.gelu(dot(a_ref[...], w1_ref[...]), approximate=True).astype(BF16)
    acc_ref[...] += dot(hid, w2_ref[...])

    @pl.when(step == pl.num_programs(0) - 1)
    def _():
        y = (x_ref[...].astype(F32) + gate1 * acc_ref[...]).astype(BF16)
        fin = (layer_norm(y.astype(F32)) * (1.0 + scale2) + shift2).astype(BF16)
        tok_ref[...] = dot(fin, wf_ref[...])
        rows, part = mix_ref.shape[0] // 2, wf_ref.shape[1] // 2
        tok_w = tok_ref.shape[0] // rows
        toks = [tok_ref[pl.ds(j, rows, stride=tok_w), :] for j in range(tok_w)]
        for p in range(2):
            mix_ref[pl.ds(p, rows, stride=2), :] = jnp.concatenate([t[:, p * part:(p + 1) * part] for t in toks], axis=1)
        lat_ref[...] = mix_ref[...].astype(BF16)
        net.all_here()
        copies = net.to_all(lat_ref, recv, sems)
        recv[net.strip] = mix_ref[...].astype(BF16)
        for copy in copies:
            copy.wait()
        o_ref[...] = recv[...]


def mlp(x, tok_w, mod_vec, w_fc1, w_fc2, w_final, net_shape, cid):
    n = net_shape[0] * net_shape[1]
    n_tok, d = x.shape
    hid, patch = w_fc1.shape[1], w_final.shape[1]
    blk = 512
    rows = 2 * n_tok // tok_w
    lat = (rows, n_tok * patch // rows)

    def whole(shape):
        return pl.BlockSpec(shape, lambda i: (0,) * len(shape))
    return pl.pallas_call(
        functools.partial(mlp_kernel, net_shape), grid=(hid // blk,),
        out_shape=jax.ShapeDtypeStruct((n,) + lat, BF16),
        in_specs=[whole(x.shape), whole(mod_vec.shape), pl.BlockSpec((d, blk), lambda i: (0, i)),
                  pl.BlockSpec((blk, d), lambda i: (i, 0)), whole(w_final.shape)],
        out_specs=whole((n,) + lat),
        scratch_shapes=[pltpu.VMEM(x.shape, BF16), pltpu.VMEM(x.shape, F32), pltpu.VMEM((n_tok, patch), F32),
                        pltpu.VMEM(lat, F32), pltpu.VMEM(lat, BF16), pltpu.VMEM((n,) + lat, BF16),
                        pltpu.SemaphoreType.DMA((2, n))],
        compiler_params=comm_params(cid, 60),
        name='mlp',
    )(x, mod_vec, w_fc1, w_fc2, w_final)


def in_group(channel, lane, per):
    return jnp.where((channel >= lane * per) & (channel < lane * per + per), 1.0, 0.0)


def group_sums(s1, s2):
    ch = s1.shape[1]
    shape = (ch, LANES)
    both = [exact_dot(s, in_group(iota(shape, 0), iota(shape, 1) - at, ch // GROUPS))
            for s, at in ((s1, 0), (s2, GROUPS))]
    return jnp.sum(both[0] + both[1], axis=0, keepdims=True)


def norm_coefs(tot, norm_ref, ch, count):
    avg = jnp.broadcast_to(tot / count, (8, LANES))
    shape = (LANES, ch)
    mean, square = [exact_dot(avg, in_group(iota(shape, 1), iota(shape, 0) - at, ch // GROUPS)) for at in (0, GROUPS)]
    scale = lax.rsqrt(square - jnp.square(mean) + 1e-6) * norm_ref[0:1]
    return mean[0:1], scale[0:1], norm_ref[1:2]


def fold8(v):
    return jnp.sum(v.reshape(v.shape[0] // 8, 8, v.shape[1]), axis=0)


def attention_kernel(net_shape, lat_ref, win_ref, norm_ref, wqkv_ref, wproj_ref, out_ref, tot_ref,
                     cols_ref, toe_ref, fmap_ref, loc_ref, sc_ref, s1_ref, s2_ref, m_ref, l_ref, acc_ref,
                     stat_ref, recv, sems, hrecv, hsems):
    net = Net(*net_shape)
    net.greet()
    rows = lat_ref.shape[0]
    lat_c, ch = win_ref.shape[1:]
    wid = lat_ref.shape[1] // lat_c
    own = rows // net.n
    lat = lat_ref[...].astype(F32)
    idx = iota(lat.shape, 0)
    cols_ref[:, :LANES] = jnp.where(idx == 0, 0.0, pltpu.roll(lat, 1, 0)).astype(BF16)
    cols_ref[:, LANES:2 * LANES] = lat_ref[...]
    cols_ref[:, 2 * LANES:] = jnp.where(idx == rows - 1, 0.0, pltpu.roll(lat, rows - 1, 0)).astype(BF16)
    clear(toe_ref)
    for x in range(wid):
        for tap in range(9):
            src = x + tap % 3 - 1
            if 0 <= src < wid:
                toe_ref[x, pl.ds(tap // 3 * LANES + src * lat_c, lat_c), :] = win_ref[tap]
    clear(s1_ref, s2_ref)
    blk = 256
    per_col = rows // blk

    def conv_step(i, carry):
        y = dot(cols_ref[aligned(lax.rem(i, per_col) * blk, blk, blk), :], toe_ref[i // per_col]).astype(BF16)
        fmap_ref[aligned(i * blk, blk, blk), :] = y
        yf = y.astype(F32)
        s1_ref[...] += fold8(yf)
        s2_ref[...] += fold8(yf * yf)
        return carry
    lax.fori_loop(0, wid * per_col, conv_step, 0)
    mean, scale, shift = norm_coefs(group_sums(s1_ref[...], s2_ref[...]), norm_ref, ch, float(rows * wid * (ch // GROUPS)))

    for x in range(wid):
        loc_ref[x * own:(x + 1) * own, :] = fmap_ref[aligned(x * rows + net.strip * own, own, own), :]
    few = 64

    def norm_step(i, carry):
        r = aligned(i * few, few, few)
        fmap_ref[r, :] = ((fmap_ref[r, :].astype(F32) - mean) * scale + shift).astype(BF16)
        return carry
    lax.fori_loop(0, rows * wid // few, norm_step, 0, unroll=2)

    nl = ((loc_ref[...].astype(F32) - mean) * scale + shift).astype(BF16)
    q = dot(nl, wqkv_ref[:, :ch]).astype(BF16)
    qk = dot_t(q, wqkv_ref[:, ch:2 * ch]).astype(BF16)
    nk, n_q, kb = sc_ref.shape
    m_ref[...] = jnp.full_like(m_ref, -jnp.inf)

    def score_step(i, carry):
        s = dot_t(qk, fmap_ref[aligned(i * kb, kb, kb), :]) * (float(ch) ** -0.5)
        sc_ref[i] = s
        m = m_ref[...]
        for j in range(kb // LANES):
            m = jnp.maximum(m, s[:, j * LANES:(j + 1) * LANES])
        m_ref[...] = m
        return carry
    lax.fori_loop(0, nk, score_step, 0)
    m_ref[...] = jnp.broadcast_to(jnp.max(m_ref[...], axis=1, keepdims=True), m_ref.shape)
    clear(l_ref, acc_ref)

    def value_step(i, carry):
        m = m_ref[...]
        tot_l = l_ref[...]
        parts = []
        for j in range(kb // LANES):
            e = jnp.exp(sc_ref[i, :, j * LANES:(j + 1) * LANES] - m)
            tot_l = tot_l + e
            parts.append(e.astype(BF16))
        l_ref[...] = tot_l
        acc_ref[...] += dot(jnp.concatenate(parts, axis=1), fmap_ref[aligned(i * kb, kb, kb), :])
        return carry
    lax.fori_loop(0, nk, value_step, 0)
    pn = (acc_ref[...] / jnp.sum(l_ref[...], axis=1, keepdims=True)).astype(BF16)
    att = dot(pn, wqkv_ref[:, 2 * ch:]).astype(BF16)
    out = (loc_ref[...].astype(F32) + dot(att, wproj_ref[...])).astype(BF16)
    i, j = iota((n_q, n_q), 0), iota((n_q, n_q), 1)
    perm = jnp.where(j == lax.rem(i, wid) * own + i // wid, 1.0, 0.0).astype(BF16)
    of = dot(perm, out)
    out_ref[pl.ds(1, own)] = of.astype(BF16).reshape(own, wid, ch)
    exchange(net, group_sums(fold8(of), fold8(of * of)), stat_ref, recv, sems, tot_ref,
             (out_ref.at[1], out_ref.at[own], hrecv, hsems, out_ref.at[0], out_ref.at[own + 1]))


def attention(lat, conv_in, norm, w_qkv, w_proj, net_shape, cid):
    n = net_shape[0] * net_shape[1]
    rows = lat.shape[0]
    lat_c, ch = conv_in.shape[2:]
    wid = lat.shape[1] // lat_c
    own = rows // n
    n_q = own * wid
    kb = 512
    return pl.pallas_call(
        functools.partial(attention_kernel, net_shape),
        out_shape=[jax.ShapeDtypeStruct((own + 2, wid, ch), BF16), TOTALS],
        in_specs=[VMEM_SPEC] * 5, out_specs=[VMEM_SPEC] * 2,
        scratch_shapes=[pltpu.VMEM((rows, 3 * LANES), BF16), pltpu.VMEM((wid, 3 * LANES, ch), BF16),
                        pltpu.VMEM((rows * wid, ch), BF16), pltpu.VMEM((n_q, ch), BF16),
                        pltpu.VMEM((rows * wid // kb, n_q, kb), F32),
                        *sum_scratch(ch),
                        pltpu.VMEM((n_q, LANES), F32), pltpu.VMEM((n_q, LANES), F32), pltpu.VMEM((n_q, ch), F32)]
        + net_scratch(n, (wid, ch)),
        compiler_params=comm_params(cid, 36),
        name='attention',
    )(lat, conv_in.reshape(9, lat_c, ch), norm, w_qkv, w_proj)


def side_by_side(y, wid):
    n_px = y.shape[0]
    col = lax.rem(iota(y.shape, 0), wid)
    return (jnp.where(col == 0, 0.0, pltpu.roll(y, 1, 0)), y,
            jnp.where(col == wid - 1, 0.0, pltpu.roll(y, n_px - 1, 0)))


class Rows:
    def __init__(self, net, x_ref, coefs, wid, h, pad, n_out, blk, pair):
        self.net, self.x_ref, self.coefs, self.wid, self.h, self.pad = net, x_ref, coefs, wid, h, pad
        self.n_out, self.blk, self.pair = n_out, blk, pair
        self.ch = x_ref.shape[-1]

    def start(self, b):
        return jnp.minimum(b * self.blk, self.n_out - self.blk) if self.n_out > self.blk else 0

    def inside(self, row):
        net = self.net
        return ((row >= self.pad) | (net.strip > 0)) & ((row < self.h + self.pad) | (net.strip < net.n - 1))

    def fill(self, buf, b):
        mean, scale, shift = self.coefs
        wid, ch, k0 = self.wid, self.ch, self.start(b)
        together = max(1, 16 // wid)
        for j in range(0, self.blk + 2, together):
            row = k0 + j
            v = self.x_ref[aligned(row * wid, together * wid, 8), :].astype(F32)
            if together == 1:
                keep = jnp.where(self.inside(row), 1.0, 0.0)
                y = silu((v - mean) * (scale * keep) + shift * keep)
            else:
                y = silu((v - mean) * scale + shift)
                y = jnp.where(self.inside(row + iota(y.shape, 0) // wid), y, 0.0)
            for lane, part in enumerate(side_by_side(y, wid)):
                lanes = slice(lane * ch, (lane + 1) * ch)
                if self.pair:
                    buf[j % 2, j // 2 * wid:(j // 2 + 1) * wid, lanes] = part.astype(buf.dtype)
                else:
                    buf[j * wid:(j + together) * wid, lanes] = part.astype(buf.dtype)

    def buffer(self):
        n_px, ch = (self.blk + 2) * self.wid, self.ch
        shape = (2, n_px // 2, 3 * ch) if self.pair else (n_px, 3 * ch)
        return pltpu.VMEM(shape, F32 if self.wid < 16 else BF16)

    def product(self, buf, w_ref):
        acc = None
        m = self.blk * self.wid // (2 if self.pair else 1)
        for t in range(4 if self.pair else 3):
            if self.pair:
                lhs = buf[t % 2, t // 2 * self.wid:t // 2 * self.wid + m, :]
            else:
                lhs = buf[t * self.wid:t * self.wid + m, :].astype(BF16)
            part = dot(lhs, w_ref[t])
            acc = part if acc is None else acc + part
        return acc

    def run(self, bufs, work):
        n_blk = -(-self.n_out // self.blk)
        self.fill(bufs[0], 0)
        if n_blk > 1:
            def step(i, carry):
                self.fill(bufs[1], 2 * i + 1)
                work(bufs[0], 2 * i)
                self.fill(bufs[0], 2 * i + 2)
                work(bufs[1], 2 * i + 1)
                return carry
            lax.fori_loop(0, n_blk // 2, step, 0)
        if n_blk % 2:
            work(bufs[0], n_blk - 1)


def paired_weights(w_ref, wp_ref):
    oc = w_ref.shape[2]
    clear(wp_ref)
    for t in range(3):
        wp_ref[t, :, :oc] = w_ref[t]
        wp_ref[t + 1, :, oc:] = w_ref[t]


def conv_kernel(cfg, *refs):
    net_shape, wid, h, blk, out_ext, pair, shortcut, stats, edge = cfg
    refs = list(refs)
    x_ref, norm_tot_ref, norm_ref, w_ref = refs[:4]
    del refs[:4]
    short_ref = refs.pop(0) if shortcut else None
    skip_ref = refs.pop(0) if shortcut == 'matmul' else None
    out_ref = refs.pop(0)
    tot_ref = refs.pop(0) if stats else None
    buf0, buf1, s1_ref, s2_ref = refs[:4]
    del refs[:4]
    wp_ref = refs.pop(0) if pair else w_ref
    net = Net(*net_shape)
    if stats:
        net.greet()
    ch, oc = x_ref.shape[-1], w_ref.shape[2]
    n_out = h + 2 * out_ext
    coefs = norm_coefs(norm_tot_ref[...], norm_ref, ch, float(net.n * h * wid * (ch // GROUPS)))
    rows = Rows(net, x_ref, coefs, wid, h, 1 + out_ext, n_out, blk, pair)
    clear(s1_ref, s2_ref)
    if pair:
        paired_weights(w_ref, wp_ref)
    exact = n_out % blk == 0 and not out_ext

    def count(y, first_row, b, step):
        yf = y.astype(F32)
        if not exact:
            r = first_row + step * (iota(yf.shape, 0) // wid)
            yf = jnp.where((r >= out_ext) & (r < h + out_ext) & (r >= b * blk), yf, 0.0)
        s1_ref[...] += fold8(yf)
        s2_ref[...] += fold8(yf * yf)

    def work(buf, b):
        k0 = rows.start(b)
        acc = rows.product(buf, wp_ref)
        if pair:
            for a in range(2):
                val = acc[:, a * oc:(a + 1) * oc]
                here = pl.ds(edge // 2 + k0 // 2, blk // 2)
                if shortcut:
                    src = short_ref[pl.ds(k0 // 2, blk // 2), a]
                    val = dot(src.reshape(blk // 2 * wid, src.shape[-1]), skip_ref[...]) + val
                y = val.astype(BF16)
                out_ref[here, a] = y.reshape(blk // 2, wid, oc)
                if stats:
                    count(y, k0 + a, b, 2)
        else:
            if shortcut == 'same':
                acc = short_ref[aligned(k0 * wid, blk * wid, 8), :].astype(F32) + acc
            elif shortcut == 'matmul':
                acc = dot(short_ref[aligned(k0 * wid, blk * wid, 8), :], skip_ref[...]) + acc
            y = acc.astype(BF16)
            out_ref[aligned((k0 + edge) * wid, blk * wid, 8), :] = y
            if stats:
                count(y, k0, b, 1)
    rows.run((buf0, buf1), work)
    if out_ext:
        for at, at_edge in ((0, net.strip == 0), (n_out - 1, net.strip == net.n - 1)):
            where = out_ref.at[at // 2, at % 2] if pair else out_ref.at[pl.ds(at * wid, wid)]

            @pl.when(at_edge)
            def _():
                where[...] = jnp.zeros(where.shape, BF16)
    if stats:
        sides = None
        if edge:
            def part(row):
                return out_ref.at[row // 2] if pair else out_ref.at[pl.ds(row * wid, edge * wid)]
            sides = (part(edge), part(h), refs[3], refs[4], part(0), part(h + edge))
        exchange(net, group_sums(s1_ref[...], s2_ref[...]), *refs[:3], tot_ref, sides)


def conv(x, tot, norm, w, h, wid, net_shape, blk, out_ext=0, short=None, skip=None, stats=False, edge=0, pair=False, cid=None):
    n = net_shape[0] * net_shape[1]
    ch, oc = w.shape[2:]
    args = [x, tot, norm, w.reshape(3, 3 * ch, oc)]
    kind = None
    if short is not None:
        kind = 'same' if skip is None else 'matmul'
        args.append(short.reshape(-1, 2, wid, short.shape[-1]) if pair else short)
        args += [] if skip is None else [skip]
    n_out = h + 2 * out_ext
    rows = n_out + 2 * edge
    outs = [jax.ShapeDtypeStruct((rows // 2, 2, wid, oc) if pair else (rows * wid, oc), BF16)]
    if stats:
        outs.append(TOTALS)
    cfg = (net_shape, wid, h, blk, out_ext, pair, kind, stats, edge)
    layout = Rows(None, x, None, wid, h, None, n_out, blk, pair)
    scratch = [layout.buffer(), layout.buffer(), *sum_scratch(oc)]
    if pair:
        scratch.append(pltpu.VMEM((4, 3 * ch, 2 * oc), BF16))
    if stats:
        scratch += net_scratch(n, ((2, wid, oc) if pair else (edge * wid, oc)) if edge else None)
    px = n_out * wid
    res = pl.pallas_call(
        functools.partial(conv_kernel, cfg),
        out_shape=outs, in_specs=[VMEM_SPEC] * len(args), out_specs=[VMEM_SPEC] * len(outs),
        scratch_shapes=scratch,
        compiler_params=comm_params(cid, 28) if stats else pltpu.CompilerParams(vmem_limit_bytes=28 * MIB),
        cost_estimate=pl.CostEstimate(flops=18 * ch * oc * px, bytes_accessed=2 * px * (ch + oc), transcendentals=px * ch),
        name='conv_w%d_%d_%d' % (wid, ch, oc) + ('e' if out_ext else ''),
    )(*args)
    return [res[0].reshape(rows * wid, oc)] + list(res[1:])


def upconv_kernel(cfg, x_ref, w_ref, out_ref, tot_ref, s1_ref, s2_ref, mix_ref, stat_ref, recv, sems):
    net_shape, half, hs, blk = cfg
    net = Net(*net_shape)
    net.greet()
    oc = w_ref.shape[2]
    n_k = hs + 1
    m, more = blk * half, (blk + 1) * half
    clear(s1_ref, s2_ref)

    def step(b, carry):
        k0 = jnp.minimum(b * blk, n_k - blk) if n_k > blk else 0
        x = x_ref[aligned(k0 * half, more, 8), :]
        col = lax.rem(iota((m, oc), 0), half)
        rows = []
        for dx in range(3):
            above, mid, below = [dot(x, w_ref[3 * dy + dx]) for dy in range(3)]
            both = above[:m] + below[half:]
            rows.append((both + mid[:m], both + mid[half:]))
        for a in range(2):
            left, at, right = [r[a] for r in rows]
            even = at + right + jnp.where(col == 0, 0.0, pltpu.roll(left, 1, 0))
            odd = left + at + jnp.where(col == half - 1, 0.0, pltpu.roll(right, m - 1, 0))
            k = k0 + iota((m, oc), 0) // half
            own = (k >= b * blk) & ((k >= 1) if a == 0 else (k < hs))
            for q, val in ((0, even), (1, odd)):
                yf = val.astype(BF16).astype(F32)
                for c in range(0, oc, LANES):
                    mix_ref[a, c // LANES, pl.ds(q, m, stride=2), :] = yf[:, c:c + LANES]
                yf = jnp.where(own, yf, 0.0)
                s1_ref[...] += fold8(yf)
                s2_ref[...] += fold8(yf * yf)
            for c in range(0, oc, LANES):
                out_ref[pl.ds(k0, blk), a, :, c:c + LANES] = mix_ref[a, c // LANES].astype(BF16).reshape(blk, 2 * half, LANES)
        return carry
    if n_k == blk:
        step(0, 0)
    else:
        lax.fori_loop(0, -(-n_k // blk), step, 0)
    exchange(net, group_sums(s1_ref[...], s2_ref[...]), stat_ref, recv, sems, tot_ref)


def upconv(x, w, hs, half, net_shape, blk, cid):
    n = net_shape[0] * net_shape[1]
    ch, oc = w.shape[2:]
    px = 4 * (hs + 1) * half
    out, tot = pl.pallas_call(
        functools.partial(upconv_kernel, (net_shape, half, hs, blk)),
        out_shape=[jax.ShapeDtypeStruct((hs + 1, 2, 2 * half, oc), BF16), TOTALS],
        in_specs=[VMEM_SPEC] * 2, out_specs=[VMEM_SPEC] * 2,
        scratch_shapes=[*sum_scratch(oc),
                        pltpu.VMEM((2, oc // LANES, 2 * blk * half, LANES), F32)] + net_scratch(n),
        compiler_params=comm_params(cid, 28),
        cost_estimate=pl.CostEstimate(flops=5 * ch * oc * px, bytes_accessed=2 * px * (ch + oc), transcendentals=0),
        name='upconv_w%d' % (2 * half),
    )(x, w.reshape(9, ch, oc))
    return out.reshape(px, oc), tot


def last_kernel(cfg, x_ref, tot_ref, norm_ref, w_ref, out_ref, z_ref, buf0, buf1):
    net_shape, wid, h, blk = cfg
    net = Net(*net_shape)
    ch = x_ref.shape[1]
    coefs = norm_coefs(tot_ref[...], norm_ref, ch, float(net.n * h * wid * (ch // GROUPS)))
    rows = Rows(net, x_ref, coefs, wid, h, 1, h, blk, False)
    m = blk * wid

    def work(buf, b):
        z = dot_t(w_ref[...], buf[...])
        out_ref[:, aligned(b * m, m, LANES)] = z[:8, :m] + z[8:16, wid:wid + m] + z[16:, 2 * wid:2 * wid + m]
    rows.run((buf0, buf1), work)


def last_conv(x, tot, norm, w, h, wid, net_shape, blk):
    ch, oc = w.shape[2:]
    wt = jnp.zeros((3, 8, 3 * ch), BF16).at[:, :oc].set(w.reshape(3, 3 * ch, oc).transpose(0, 2, 1))
    layout = Rows(None, x, None, wid, h, None, h, blk, False)
    return pl.pallas_call(
        functools.partial(last_kernel, (net_shape, wid, h, blk)),
        out_shape=jax.ShapeDtypeStruct((8, h * wid), F32),
        in_specs=[VMEM_SPEC] * 4, out_specs=VMEM_SPEC,
        scratch_shapes=[pltpu.VMEM((8, LANES), F32), layout.buffer(), layout.buffer()],
        compiler_params=pltpu.CompilerParams(vmem_limit_bytes=28 * MIB),
        name='last_conv',
    )(x, tot, norm, wt.reshape(-1, 3 * ch))


def device_body(net_shape, tokens, mod_vec, w_fc1, w_fc2, w_final, conv_in, norm_attn, w_qkv, w_proj,
                norm0_a, conv0_a, norm0_b, conv0_b, upconv_0, norm1_a, conv1_a, norm1_b, conv1_b, upconv_1,
                norm2_a, conv2_a, norm2_b, conv2_b, skip_2, upconv_2, norm3_a, conv3_a, norm3_b, conv3_b,
                skip_3, norm_out, conv_out):
    n_col = net_shape[1]
    trows, tok_w, d = tokens.shape
    full = mlp(tokens.reshape(-1, d), tok_w, mod_vec, w_fc1, w_fc2, w_final, net_shape, 1)
    h, wid = 2 * trows, 2 * tok_w
    f, tot = attention(full.reshape(-1, full.shape[-1]), conv_in, norm_attn, w_qkv, w_proj, net_shape, 2)
    u = f.reshape(-1, f.shape[-1])
    blocks = [(norm0_a, conv0_a, norm0_b, conv0_b, None, upconv_0, h, h + 2, h + 1),
              (norm1_a, conv1_a, norm1_b, conv1_b, None, upconv_1, 16, 11, 13),
              (norm2_a, conv2_a, norm2_b, conv2_b, skip_2, upconv_2, 8, 10, 10),
              (norm3_a, conv3_a, norm3_b, conv3_b, skip_3, None, 8, 16, None)]
    cid = 3
    for norm_a, conv_a, norm_b, conv_b, skip, up, blk_a, blk_b, blk_up in blocks:
        last = up is None
        g, tot = conv(u, tot, norm_a, conv_a, h, wid, net_shape, blk_a, stats=True, edge=2, pair=last, cid=cid)
        f, *tot = conv(g, tot, norm_b, conv_b, h, wid, net_shape, blk_b, out_ext=1, short=u, skip=skip,
                       stats=last, pair=last, cid=cid + 1)
        if not last:
            u, tot = upconv(f, up, h, wid, net_shape, blk_up, cid + 2)
            h, wid = 2 * h, 2 * wid
        cid += 3
    rgb = last_conv(f, tot[0], norm_out, conv_out, h, wid, net_shape, 16)[:conv_out.shape[3]]
    tw = wid // n_col
    out = rgb.reshape(-1, h, n_col, tw).transpose(2, 0, 1, 3).reshape(n_col, -1, h * tw)
    back = lax.all_to_all(out, 'col', 0, 0, tiled=True)
    return back.reshape(n_col, -1, h, tw).transpose(0, 2, 3, 1).reshape(n_col * h, tw, -1)


def solution(mesh):
    body_fn = functools.partial(device_body, (mesh.shape['row'], mesh.shape['col']))
    tok_spec = P(('batch', 'row', 'col'), None, None)
    out_spec = P(('batch', 'row'), 'col', None)
    return jax.shard_map(body_fn, mesh=mesh, in_specs=(tok_spec,) + (P(),) * 31, out_specs=out_spec, check_vma=False)
```

```python
import functools
import jax
import jax.numpy as jnp
from jax import lax
from jax.experimental import pallas as pl
from jax.experimental.pallas import tpu as pltpu
from jax.sharding import PartitionSpec as P

GROUPS = 32
LOG2_E = 1.4426950408889634
LANES = 128
BASE = 16
F32, BF16 = jnp.float32, jnp.bfloat16
MESH = pl.DeviceIdType.MESH
VMEM_SPEC = pl.BlockSpec(memory_space=pltpu.VMEM)
MIB = 1 << 20
TOTALS = jax.ShapeDtypeStruct((1, LANES), F32)


def dot(a, b):
    return jnp.dot(a, b, preferred_element_type=F32)


def dot_t(a, b):
    return lax.dot_general(a, b, (((1,), (1,)), ((), ())), preferred_element_type=F32)


def exact_dot(a, b):
    return jnp.dot(a, b, preferred_element_type=F32, precision=lax.Precision.HIGHEST)


def clear(*refs):
    for ref in refs:
        ref[...] = jnp.zeros_like(ref)


def iota(shape, dim):
    return lax.broadcasted_iota(jnp.int32, shape, dim)


def aligned(first, size, unit):
    return pl.ds(pl.multiple_of(first, unit), size)


def layer_norm(v):
    mean = jnp.mean(v, axis=-1, keepdims=True)
    var = jnp.mean(jnp.square(v - mean), axis=-1, keepdims=True)
    return (v - mean) * lax.rsqrt(var + 1e-6)


def silu_of_half(half):
    return half + half * jnp.tanh(half)


class Net:
    def __init__(self, n_row, n_col):
        self.n_row, self.n_col = n_row, n_col
        self.n = n_row * n_col
        self.row, self.col = lax.axis_index('row'), lax.axis_index('col')
        self.strip = self.row * n_col + self.col

    def for_others(self, act, row_step=1):
        cols = [lax.rem(self.col + k, self.n_col) for k in range(self.n_col)]
        for col in cols[1:]:
            act({'row': self.row, 'col': col})

        def step(k, carry):
            row = lax.rem(self.row + k * row_step, self.n_row)
            for col in cols:
                act({'row': row, 'col': col})
            return carry
        lax.fori_loop(1, self.n_row // row_step, step, 0)
        return self.n // row_step - 1

    def beside(self, ahead):
        other = lax.rem(self.strip + ahead, self.n)
        return {'row': other // self.n_col, 'col': lax.rem(other, self.n_col)}

    def greet(self):
        barrier = pltpu.get_barrier_semaphore()
        self.for_others(lambda device: pl.semaphore_signal(barrier, inc=1, device_id=device, device_id_type=MESH))

    def all_here(self):
        pl.semaphore_wait(pltpu.get_barrier_semaphore(), self.n - 1)

    def to_others(self, src, recv, sems, row_step=1):
        count = self.for_others(lambda device: send(src, recv.at[self.strip], sems, device).start(), row_step)

        def wait():
            done = recv.at[pl.ds(0, count)]
            for side in range(2):
                pltpu.make_async_copy(done, done, sems.at[side]).wait()
        return wait


def send(src, dst, sems, device):
    return pltpu.make_async_remote_copy(
        src_ref=src, dst_ref=dst, send_sem=sems.at[0], recv_sem=sems.at[1], device_id=device, device_id_type=MESH)


PAIR_SEM = pltpu.SemaphoreType.DMA((2,))


def net_scratch(n, edge_shape=None):
    scratch = [pltpu.VMEM((1, LANES), F32), pltpu.VMEM((n, 1, LANES), F32), PAIR_SEM]
    if edge_shape is not None:
        scratch += [pltpu.VMEM((2,) + edge_shape, BF16), PAIR_SEM, PAIR_SEM]
    return scratch


def exchange(net, stat, stat_ref, recv, sems, tot_ref, sides=None):
    stat_ref[...] = stat
    net.all_here()
    wait = net.to_others(stat_ref, recv, sems)
    side_copies = []
    if sides is not None:
        first, last, top, bottom, hrecv, down_sems, up_sems = sides
        side_copies = [(send(src, hrecv.at[side], pair, net.beside(ahead)), dst, side) for side, (src, dst, pair, ahead)
                       in enumerate(((last, top, down_sems, 1), (first, bottom, up_sems, net.n - 1)))]
    for copy, _, _ in side_copies:
        copy.start()
    recv[net.strip] = stat
    wait()
    tot_ref[...] = jnp.sum(recv[...], axis=0)
    for copy, dst, side in side_copies:
        copy.wait()
        dst[...] = hrecv[side]


def sum_scratch(ch):
    return [pltpu.VMEM((8, ch), F32)] * 2


def comm_params(cid, mib):
    return pltpu.CompilerParams(collective_id=cid, has_side_effects=True, vmem_limit_bytes=mib * MIB)


def mlp_kernel(net_shape, x_ref, mod_ref, w1_ref, w2_ref, wf_ref, o_ref,
               w1_buf, w2_buf, act_ref, acc_ref, tok_ref, mix_ref, recv, w_sems, sems, pass_sems):
    net = Net(*net_shape)
    n_buf, blk = w1_buf.shape[0], w1_buf.shape[2]
    n_cut = w1_ref.shape[1] // blk

    def loads(i):
        part, slot = aligned(i * blk, blk, blk), lax.rem(i, n_buf)
        return [pltpu.make_async_copy(w1_ref.at[:, part], w1_buf.at[slot], w_sems.at[0, slot]),
                pltpu.make_async_copy(w2_ref.at[part], w2_buf.at[slot], w_sems.at[1, slot])]
    for i in range(n_buf - 1):
        for load in loads(i):
            load.start()
    net.greet()
    shift1, scale1, gate1, shift2, scale2 = [mod_ref[pl.ds(i, 1)] for i in range(5)]
    x = x_ref[...].astype(F32)
    act = (layer_norm(x) * (1.0 + scale1) + shift1).astype(BF16)
    act_ref[...] = act
    clear(acc_ref)

    def step(i, carry):
        @pl.when(i + n_buf - 1 < n_cut)
        def _():
            for load in loads(i + n_buf - 1):
                load.start()
        load1, load2 = loads(i)
        slot = lax.rem(i, n_buf)
        load1.wait()
        hid = jax.nn.gelu(dot(act_ref[...], w1_buf[slot]), approximate=True).astype(BF16)
        load2.wait()
        acc_ref[...] += dot(hid, w2_buf[slot])
        return carry
    lax.fori_loop(0, n_cut, step, 0)
    acc = acc_ref[...]
    y = (x + gate1 * acc).astype(BF16)
    fin = (layer_norm(y.astype(F32)) * (1.0 + scale2) + shift2).astype(BF16)
    tok_ref[...] = dot_t(fin, wf_ref[...])
    rows, part = mix_ref.shape[0] // 2, wf_ref.shape[0] // 2
    tok_w = tok_ref.shape[0] // rows
    toks = [tok_ref[pl.ds(j, rows, stride=tok_w), :] for j in range(tok_w)]
    for p in range(2):
        mix_ref[pl.ds(p, rows, stride=2), :] = jnp.concatenate([t[:, p * part:(p + 1) * part] for t in toks], axis=1)
    recv[net.strip] = mix_ref[...].astype(BF16)
    net.all_here()
    net.to_others(recv.at[net.strip], recv, sems, 2)()
    core = lax.rem(net.row, 2)
    copies = []
    for i in range(net.n_row // 2):
        line = recv.at[pl.ds((2 * i + core) * net.n_col, net.n_col)]
        copies.append(send(line, line, pass_sems.at[i], {'row': net.row + 1 - 2 * core, 'col': net.col}))
        copies[-1].start()
    for copy in copies:
        copy.wait()
    o_ref[...] = recv[...]


def mlp(x, tok_w, mod_vec, w_fc1, w_fc2, w_final, net_shape, cid):
    n = net_shape[0] * net_shape[1]
    n_tok, d = x.shape
    hid, patch = w_fc1.shape[1], w_final.shape[1]
    n_buf, blk = 4, 768
    rows = 2 * n_tok // tok_w
    lat = (rows, n_tok * patch // rows)
    hbm = pl.BlockSpec(memory_space=pltpu.HBM)
    return pl.pallas_call(
        functools.partial(mlp_kernel, net_shape),
        out_shape=jax.ShapeDtypeStruct((n,) + lat, BF16),
        in_specs=[VMEM_SPEC, VMEM_SPEC, hbm, hbm, VMEM_SPEC],
        out_specs=VMEM_SPEC,
        scratch_shapes=[pltpu.VMEM((n_buf, d, blk), BF16), pltpu.VMEM((n_buf, blk, d), BF16),
                        pltpu.VMEM(x.shape, BF16), pltpu.VMEM(x.shape, F32),
                        pltpu.VMEM((n_tok, patch), F32), pltpu.VMEM(lat, F32), pltpu.VMEM((n,) + lat, BF16),
                        pltpu.SemaphoreType.DMA((2, n_buf)), PAIR_SEM, pltpu.SemaphoreType.DMA((net_shape[0] // 2, 2))],
        compiler_params=comm_params(cid, 48),
        name='mlp',
    )(x, mod_vec, w_fc1, w_fc2, w_final.T)


def in_group(channel, lane, per):
    return ((channel >= lane * per) & (channel < lane * per + per)).astype(F32)


def group_sums(s1, s2):
    ch = s1.shape[1]
    shape = (ch, LANES)
    both = [exact_dot(s, in_group(iota(shape, 0), iota(shape, 1) - at, ch // GROUPS))
            for s, at in ((s1, 0), (s2, GROUPS))]
    return jnp.sum(both[0] + both[1], axis=0, keepdims=True)


def norm_coefs(tot, norm_ref, ch, count):
    avg = jnp.broadcast_to(tot / count, (8, LANES))
    shape = (LANES, ch)
    mean, square = [exact_dot(avg, in_group(iota(shape, 1), iota(shape, 0) - at, ch // GROUPS)) for at in (0, GROUPS)]
    scale = lax.rsqrt(square - jnp.square(mean) + 1e-6) * norm_ref[0:1]
    return mean[0:1], scale[0:1], norm_ref[1:2]


def fold8(v):
    return jnp.sum(v.reshape(v.shape[0] // 8, 8, v.shape[1]), axis=0)


def attention_kernel(net_shape, lat_ref, win_ref, norm_ref, wqkv_ref, wproj_ref, out_ref, tot_ref,
                     cols_ref, toe_ref, fmap_ref, loc_ref, sc_ref, s1_ref, s2_ref, m_ref, l_ref, acc_ref,
                     stat_ref, recv, sems, *halo_refs):
    net = Net(*net_shape)
    net.greet()
    rows = lat_ref.shape[0]
    lat_c, ch = win_ref.shape[1:]
    wid = lat_ref.shape[1] // lat_c
    own = rows // net.n
    lat = lat_ref[...].astype(F32)
    idx = iota(lat.shape, 0)
    cols_ref[...] = jnp.concatenate([jnp.where(idx == 0, 0.0, pltpu.roll(lat, 1, 0)), lat,
                                     jnp.where(idx == rows - 1, 0.0, pltpu.roll(lat, rows - 1, 0))], axis=1).astype(BF16)
    clear(toe_ref)
    for x in range(wid):
        for tap in range(9):
            src = x + tap % 3 - 1
            if 0 <= src < wid:
                toe_ref[x, pl.ds(tap // 3 * LANES + src * lat_c, lat_c), :] = win_ref[tap]
    clear(s1_ref, s2_ref)
    blk = 256
    per_col = rows // blk

    def conv_step(i, carry):
        y = dot(cols_ref[aligned(lax.rem(i, per_col) * blk, blk, blk), :], toe_ref[i // per_col]).astype(BF16)
        fmap_ref[aligned(i * blk, blk, blk), :] = y
        yf = y.astype(F32)
        s1_ref[...] += fold8(yf)
        s2_ref[...] += fold8(yf * yf)
        return carry
    lax.fori_loop(0, wid * per_col, conv_step, 0)
    mean, scale, shift = norm_coefs(group_sums(s1_ref[...], s2_ref[...]), norm_ref, ch, float(rows * wid * (ch // GROUPS)))

    for x in range(wid):
        loc_ref[x * own:(x + 1) * own, :] = fmap_ref[aligned(x * rows + net.strip * own, own, own), :]
    nl = ((loc_ref[...].astype(F32) - mean) * scale + shift).astype(BF16)
    q = dot(nl, wqkv_ref[:, :ch]).astype(BF16)
    qk = (dot_t(q, wqkv_ref[:, ch:2 * ch]) * (scale * (float(ch) ** -0.5 * LOG2_E))).astype(BF16)
    nk, n_q, kb = sc_ref.shape
    m_ref[...] = jnp.full_like(m_ref, -jnp.inf)

    def score_step(i, carry):
        s = dot_t(qk, fmap_ref[aligned(i * kb, kb, kb), :])
        sc_ref[i] = s
        m = m_ref[...]
        for j in range(kb // LANES):
            m = jnp.maximum(m, s[:, j * LANES:(j + 1) * LANES])
        m_ref[...] = m
        return carry
    lax.fori_loop(0, nk, score_step, 0)
    m_ref[...] = jnp.broadcast_to(jnp.max(m_ref[...], axis=1, keepdims=True), m_ref.shape)
    clear(l_ref, acc_ref)

    def value_step(i, carry):
        m = m_ref[...]
        tot_l = l_ref[...]
        parts = []
        for j in range(kb // LANES):
            e = jnp.exp2(sc_ref[i, :, j * LANES:(j + 1) * LANES] - m).astype(BF16)
            tot_l = tot_l + e.astype(F32)
            parts.append(e)
        l_ref[...] = tot_l
        acc_ref[...] += dot(jnp.concatenate(parts, axis=1), fmap_ref[aligned(i * kb, kb, kb), :])
        return carry
    lax.fori_loop(0, nk, value_step, 0)
    pn = acc_ref[...] / jnp.sum(l_ref[...], axis=1, keepdims=True)
    pn = ((pn - mean) * scale + shift).astype(BF16)
    att = dot(pn, wqkv_ref[:, 2 * ch:]).astype(BF16)
    out = (loc_ref[...].astype(F32) + dot(att, wproj_ref[...])).astype(BF16)
    i, j = iota((n_q, n_q), 0), iota((n_q, n_q), 1)
    perm = (j == lax.rem(i, wid) * own + i // wid).astype(BF16)
    of = dot(perm, out)
    out_ref[pl.ds(1, own)] = of.astype(BF16).reshape(own, wid, ch)
    exchange(net, group_sums(fold8(of), fold8(of * of)), stat_ref, recv, sems, tot_ref,
             (out_ref.at[1], out_ref.at[own], out_ref.at[0], out_ref.at[own + 1], *halo_refs))


def attention(lat, conv_in, norm, w_qkv, w_proj, net_shape, cid):
    n = net_shape[0] * net_shape[1]
    rows = lat.shape[0]
    lat_c, ch = conv_in.shape[2:]
    wid = lat.shape[1] // lat_c
    own = rows // n
    n_q = own * wid
    kb = 512
    return pl.pallas_call(
        functools.partial(attention_kernel, net_shape),
        out_shape=[jax.ShapeDtypeStruct((own + 2, wid, ch), BF16), TOTALS],
        in_specs=[VMEM_SPEC] * 5, out_specs=[VMEM_SPEC] * 2,
        scratch_shapes=[pltpu.VMEM((rows, 3 * LANES), BF16), pltpu.VMEM((wid, 3 * LANES, ch), BF16),
                        pltpu.VMEM((rows * wid, ch), BF16), pltpu.VMEM((n_q, ch), BF16),
                        pltpu.VMEM((rows * wid // kb, n_q, kb), F32),
                        *sum_scratch(ch),
                        pltpu.VMEM((n_q, LANES), F32), pltpu.VMEM((n_q, LANES), F32), pltpu.VMEM((n_q, ch), F32)]
        + net_scratch(n, (wid, ch)),
        compiler_params=comm_params(cid, 27),
        name='attention',
    )(lat, conv_in.reshape(9, lat_c, ch), norm, w_qkv, w_proj)


def shifted(y, wid, by):
    n_px, ch = y.shape
    if wid > BASE:
        even, odd = jnp.split(y.reshape(n_px // wid, 2, wid // 2, ch), 2, axis=1)
        far = shifted((odd if by == 1 else even).reshape(n_px // 2, ch), wid // 2, by).reshape(even.shape)
        return jnp.concatenate([far, even] if by == 1 else [odd, far], axis=1).reshape(n_px, ch)
    tiles = pltpu.roll(y, by % n_px, 0).reshape(n_px // wid, wid // 8, 8, ch)
    at, sub = (0, 0) if by > 0 else (wid // 8 - 1, 7)
    edge = tiles[:, at:at + 1]
    edge = jnp.where(iota(edge.shape, 2) == sub, 0.0, edge)
    parts = [tiles[:, :at], edge, tiles[:, at + 1:]]
    return jnp.concatenate([p for p in parts if p.shape[1]], axis=1).reshape(n_px, ch)


class Rows:
    def __init__(self, net, x_ref, coefs, wid, h, pad, n_out, blk, pair):
        self.net, self.x_ref, self.coefs, self.wid, self.h, self.pad = net, x_ref, coefs, wid, h, pad
        self.n_out, self.blk, self.pair = n_out, blk, pair
        self.ch = x_ref.shape[-1]

    def inside(self, row):
        net = self.net
        return ((row >= self.pad) | (net.strip > 0)) & ((row < self.h + self.pad) | (net.strip < net.n - 1))

    def fill(self, buf, b, before=None):
        mean, scale, shift = self.coefs
        scale = 0.5 * scale
        shift = 0.5 * shift - mean * scale
        wid, ch, blk = self.wid, self.ch, self.blk
        if before is not None:
            self.keep_last(buf, before)
        together = -(-BASE // wid)
        for j in range(2 * (before is not None), blk + 2, together):
            row = b * blk + j
            if self.n_out > blk:
                row = jnp.minimum(row, self.n_out + 1)
            v = self.x_ref[aligned(row * wid, together * wid, 8), :].astype(F32)
            if together == 1:
                keep = jnp.where(self.inside(row), 1.0, 0.0)
                y = silu_of_half(v * (scale * keep) + shift * keep)
            else:
                y = silu_of_half(v * scale + shift)
                y = jnp.where(self.inside(row + iota(y.shape, 0) // wid), y, 0.0)
            for lane, part in enumerate((shifted(y, wid, 1), y, shifted(y, wid, -1))):
                lanes = slice(lane * ch, (lane + 1) * ch)
                self.put(buf, j, together, lanes, part.astype(buf.dtype))

    def keep_last(self, buf, before):
        wid, blk = self.wid, self.blk
        if self.pair:
            buf[:, :wid, :] = before[:, blk // 2 * wid:, :]
        else:
            buf[:2 * wid, :] = before[blk * wid:, :]

    def put(self, buf, j, together, lanes, part):
        wid = self.wid
        if self.pair:
            buf[j % 2, j // 2 * wid:(j // 2 + 1) * wid, lanes] = part
        else:
            buf[j * wid:(j + together) * wid, lanes] = part

    def buffer(self):
        n_px, ch = (self.blk + 2) * self.wid, self.ch
        shape = (2, n_px // 2, 3 * ch) if self.pair else (n_px, 3 * ch)
        return pltpu.VMEM(shape, F32 if self.wid < 16 else BF16)

    def product(self, buf, w_ref):
        acc = None
        m = self.blk * self.wid // (2 if self.pair else 1)
        for t in range(4 if self.pair else 3):
            if self.pair:
                lhs = buf[t % 2, t // 2 * self.wid:t // 2 * self.wid + m, :]
            else:
                lhs = buf[t * self.wid:t * self.wid + m, :].astype(BF16)
            part = dot(lhs, w_ref[t])
            acc = part if acc is None else acc + part
        return acc

    def run(self, bufs, work):
        n_blk = -(-self.n_out // self.blk)
        self.fill(bufs[0], 0)
        if n_blk > 1:
            def step(i, carry):
                self.fill(bufs[1], 2 * i + 1, bufs[0])
                work(bufs[0], 2 * i)
                self.fill(bufs[0], 2 * i + 2, bufs[1])
                work(bufs[1], 2 * i + 1)
                return carry
            lax.fori_loop(0, n_blk // 2, step, 0)
        if n_blk % 2:
            work(bufs[0], n_blk - 1)


def paired_weights(w_ref, wp_ref):
    oc = w_ref.shape[2]
    clear(wp_ref)
    for t in range(3):
        wp_ref[t, :, :oc] = w_ref[t]
        wp_ref[t + 1, :, oc:] = w_ref[t]


def conv_kernel(cfg, *refs):
    net_shape, wid, h, blk, out_ext, pair, shortcut, stats, edge = cfg
    refs = iter(refs)
    x_ref, norm_tot_ref, norm_ref, w_ref = [next(refs) for _ in 'abcd']
    short_ref = next(refs) if shortcut else None
    skip_ref = next(refs) if shortcut == 'matmul' else None
    out_ref = next(refs)
    tot_ref = next(refs) if stats else None
    buf0, buf1, s1_ref, s2_ref = [next(refs) for _ in 'abcd']
    wp_ref = next(refs) if pair else w_ref
    net_refs = list(refs)
    net = Net(*net_shape)
    if stats:
        net.greet()
    ch, oc = x_ref.shape[-1], w_ref.shape[2]
    n_out = h + 2 * out_ext
    coefs = norm_coefs(norm_tot_ref[...], norm_ref, ch, float(net.n * h * wid * (ch // GROUPS)))
    rows = Rows(net, x_ref, coefs, wid, h, 1 + out_ext, n_out, blk, pair)
    clear(s1_ref, s2_ref)
    if pair:
        paired_weights(w_ref, wp_ref)
    exact = n_out % blk == 0 and not out_ext

    def count(y, first_row, step):
        yf = y.astype(F32)
        if exact:
            s1_ref[...] += fold8(yf)
            s2_ref[...] += fold8(yf * yf)
            return
        for i, part in enumerate(jnp.split(yf, yf.shape[0] // wid)):
            r = first_row + step * i
            own = (r >= out_ext) & (r < h + out_ext)
            s1_ref[...] += jnp.where(own, fold8(part), 0.0)
            s2_ref[...] += jnp.where(own, fold8(part * part), 0.0)

    def work(buf, b):
        k0 = b * blk
        acc = rows.product(buf, wp_ref)
        if pair:
            for a in range(2):
                val = acc[:, a * oc:(a + 1) * oc]
                here = pl.ds(edge // 2 + k0 // 2, blk // 2)
                if shortcut:
                    src = short_ref[pl.ds(k0 // 2, blk // 2), a]
                    val = dot(src.reshape(blk // 2 * wid, src.shape[-1]), skip_ref[...]) + val
                y = val.astype(BF16)
                out_ref[here, a] = y.reshape(blk // 2, wid, oc)
                if stats:
                    count(y, k0 + a, 2)
        else:
            if shortcut == 'add':
                acc = short_ref[aligned(k0 * wid, blk * wid, 8), :].astype(F32) + acc
            elif shortcut == 'matmul':
                acc = dot(short_ref[aligned(k0 * wid, blk * wid, 8), :], skip_ref[...]) + acc
            y = acc.astype(BF16)
            out_ref[aligned((k0 + edge) * wid, blk * wid, 8), :] = y
            if stats:
                count(y, k0, 1)
    rows.run((buf0, buf1), work)
    if out_ext:
        for at, at_edge in ((0, net.strip == 0), (n_out - 1, net.strip == net.n - 1)):
            where = out_ref.at[at // 2, at % 2] if pair else out_ref.at[pl.ds(at * wid, wid)]

            @pl.when(at_edge)
            def _():
                where[...] = jnp.zeros(where.shape, BF16)
    if stats:
        sides = None
        if edge:
            def part(row):
                return out_ref.at[row // 2] if pair else out_ref.at[pl.ds(row * wid, edge * wid)]
            sides = (part(edge), part(h), part(0), part(h + edge), *net_refs[3:])
        exchange(net, group_sums(s1_ref[...], s2_ref[...]), *net_refs[:3], tot_ref, sides)


def conv(x, tot, norm, w, h, wid, net_shape, blk, out_ext, stats, edge, pair, cid, *shortcut):
    n = net_shape[0] * net_shape[1]
    ch, oc = w.shape[2:]
    args = [x, tot, norm, w.reshape(3, 3 * ch, oc)]
    for short in shortcut[:1]:
        args.append(short.reshape(-1, 2, wid, short.shape[-1]) if pair else short)
    args += shortcut[1:]
    n_out = h + 2 * out_ext
    rows = -(-n_out // blk) * blk + 2 * edge
    outs = [jax.ShapeDtypeStruct((rows // 2, 2, wid, oc) if pair else (rows * wid, oc), BF16)]
    if stats:
        outs.append(TOTALS)
    cfg = (net_shape, wid, h, blk, out_ext, pair, ('', 'add', 'matmul')[len(shortcut)], stats, edge)
    layout = Rows(None, x, None, wid, h, None, n_out, blk, pair)
    scratch = [layout.buffer(), layout.buffer(), *sum_scratch(oc)]
    if pair:
        scratch.append(pltpu.VMEM((4, 3 * ch, 2 * oc), BF16))
    if stats:
        scratch += net_scratch(n, ((2, wid, oc) if pair else (edge * wid, oc)) if edge else None)
    px = n_out * wid
    res = pl.pallas_call(
        functools.partial(conv_kernel, cfg),
        out_shape=outs, in_specs=[VMEM_SPEC] * len(args), out_specs=[VMEM_SPEC] * len(outs),
        scratch_shapes=scratch,
        compiler_params=comm_params(cid, 28) if stats else pltpu.CompilerParams(vmem_limit_bytes=28 * MIB),
        cost_estimate=pl.CostEstimate(flops=18 * ch * oc * px, bytes_accessed=2 * px * (ch + oc), transcendentals=px * ch),
        name='conv_w%d_%d_%d' % (wid, ch, oc) + ('e' if out_ext else ''),
    )(*args)
    return [res[0].reshape(rows * wid, oc)] + list(res[1:])


def upconv_kernel(cfg, x_ref, w_ref, out_ref, tot_ref, s1_ref, s2_ref, mix_ref, stat_ref, recv, sems):
    net_shape, half, hs, blk = cfg
    net = Net(*net_shape)
    net.greet()
    oc = w_ref.shape[2]
    n_k = hs + 1
    mixed = half < BASE
    m, more = blk * half, (blk + 1) * half
    clear(s1_ref, s2_ref)

    def step(b, carry):
        k0 = jnp.minimum(b * blk, n_k - blk) if n_k > blk else 0
        x = x_ref[aligned(k0 * half, more, 8), :]
        rows = []
        for dx in range(3):
            above, mid, below = [dot(x, w_ref[3 * dy + dx]) for dy in range(3)]
            both = above[:m] + below[half:]
            rows.append((both + mid[:m], both + mid[half:]))
        for a in range(2):
            left, at, right = [r[a] for r in rows]
            even = at + right + shifted(left, half, 1)
            odd = left + at + shifted(right, half, -1)
            for q, val in ((0, even), (1, odd)):
                y = val.astype(BF16)
                if mixed:
                    for c in range(0, oc, LANES):
                        mix_ref[a, c // LANES, pl.ds(q, m, stride=2), :] = val[:, c:c + LANES]
                else:
                    out_ref[pl.ds(k0, blk), a, q * half:(q + 1) * half, :] = y.reshape(blk, half, oc)
                yf = y.astype(F32)
                for i, part in enumerate(jnp.split(yf, blk)):
                    k = k0 + i
                    own = (k >= b * blk) & ((k < hs) if a else (k > 0))
                    s1_ref[...] += jnp.where(own, fold8(part), 0.0)
                    s2_ref[...] += jnp.where(own, fold8(part * part), 0.0)
            for c in range(0, oc if mixed else 0, LANES):
                out_ref[pl.ds(k0, blk), a, :, c:c + LANES] = mix_ref[a, c // LANES].astype(BF16).reshape(blk, 2 * half, LANES)
        return carry
    if n_k == blk:
        step(0, 0)
    else:
        lax.fori_loop(0, -(-n_k // blk), step, 0)
    exchange(net, group_sums(s1_ref[...], s2_ref[...]), stat_ref, recv, sems, tot_ref)


def upconv(x, w, hs, half, net_shape, blk, cid):
    n = net_shape[0] * net_shape[1]
    ch, oc = w.shape[2:]
    n_k = hs + 8
    px = 4 * n_k * half
    out, tot = pl.pallas_call(
        functools.partial(upconv_kernel, (net_shape, half, hs, blk)),
        out_shape=[jax.ShapeDtypeStruct((n_k, 2, 2 * half, oc), BF16), TOTALS],
        in_specs=[VMEM_SPEC] * 2, out_specs=[VMEM_SPEC] * 2,
        scratch_shapes=[*sum_scratch(oc),
                        pltpu.VMEM((2, oc // LANES, 2 * blk * half if half < BASE else 8, LANES), F32)] + net_scratch(n),
        compiler_params=comm_params(cid, 28),
        cost_estimate=pl.CostEstimate(flops=5 * ch * oc * px, bytes_accessed=2 * px * (ch + oc), transcendentals=0),
        name='upconv_w%d' % (2 * half),
    )(x, w.reshape(9, ch, oc))
    return out.reshape(px, oc), tot


class QuarterRows(Rows):
    def keep_last(self, buf, before):
        buf[:, :2 * self.tile] = before[:, self.blk * self.tile:]

    def put(self, buf, j, together, lanes, part):
        n_q = buf.shape[0]
        here = self.tile // (self.wid // BASE)
        whole = part.reshape(self.wid // BASE, BASE, part.shape[1])
        for q in range(n_q):
            buf[q, j * self.tile:(j + 1) * self.tile, lanes] = whole[:, q * here:(q + 1) * here].reshape(self.tile, part.shape[1])


def last_kernel(cfg, x_ref, tot_ref, norm_ref, w_ref, out_ref, buf0, buf1, mine, recv, send_sems, recv_sems):
    net_shape, wid, h, blk, oc = cfg
    net = Net(*net_shape)
    barrier = pltpu.get_barrier_semaphore()
    cols = [lax.rem(net.col + k, net.n_col) for k in range(net.n_col)]
    for col in cols[1:]:
        pl.semaphore_signal(barrier, inc=1, device_id={'col': col}, device_id_type=MESH)
    ch = x_ref.shape[1]
    coefs = norm_coefs(tot_ref[...], norm_ref, ch, float(net.n * h * wid * (ch // GROUPS)))
    rows = QuarterRows(net, x_ref, coefs, wid, h, 1, h, blk, False)
    rows.tile = tile = wid // net.n_col
    m = blk * tile
    per = h * tile // LANES

    def work(buf, b):
        for q in range(net.n_col):
            z = dot_t(w_ref[...], buf[q])
            z = z[:8, :m] + z[8:16, tile:tile + m] + z[16:, 2 * tile:2 * tile + m]
            for c in range(oc):
                for t in range(m // LANES):
                    mine[q, pl.ds(c * per + b * (m // LANES) + t, 1), :] = z[c:c + 1, t * LANES:(t + 1) * LANES]
    rows.run((buf0, buf1), work)
    pl.semaphore_wait(barrier, net.n_col - 1)
    copies = []
    for k, col in enumerate(cols[1:]):
        copies.append(pltpu.make_async_remote_copy(
            src_ref=mine.at[col], dst_ref=recv.at[net.col], send_sem=send_sems.at[k], recv_sem=recv_sems.at[k],
            device_id={'col': col}, device_id_type=MESH))
        copies[-1].start()
    recv[net.col] = mine[net.col]
    for copy in copies:
        copy.wait()
    i, j = iota((LANES, LANES), 0), iota((LANES, LANES), 1)
    splits = wid // BASE
    lane, run = lax.rem(j, tile), j // tile
    src = run * tile + lax.rem(lane, 2) * (tile // 2) + lax.rem(lane // 2, splits // 2) * (tile // splits) + lane // splits
    perm = (i == src).astype(F32)
    for q in range(net.n_col):
        out_ref[q] = exact_dot(recv[q], perm)


def last_conv(x, tot, norm, w, h, wid, net_shape, blk, cid):
    n_col = net_shape[1]
    ch, oc = w.shape[2:]
    wt = jnp.zeros((3, 8, 3 * ch), BF16).at[:, :oc].set(w.reshape(3, 3 * ch, oc).transpose(0, 2, 1))
    buf = pltpu.VMEM((n_col, (blk + 2) * wid // n_col, 3 * ch), BF16)
    shape = (n_col, oc * h * wid // n_col // LANES, LANES)
    return pl.pallas_call(
        functools.partial(last_kernel, (net_shape, wid, h, blk, oc)),
        out_shape=jax.ShapeDtypeStruct(shape, F32),
        in_specs=[VMEM_SPEC] * 4, out_specs=VMEM_SPEC,
        scratch_shapes=[buf, buf, pltpu.VMEM(shape, F32), pltpu.VMEM(shape, F32)] + [pltpu.SemaphoreType.DMA((n_col,))] * 2,
        compiler_params=comm_params(cid, 28),
        name='last_conv',
    )(x, tot, norm, wt.reshape(-1, 3 * ch))


def device_body(net_shape, tokens, mod_vec, w_fc1, w_fc2, w_final, conv_in, norm_attn, w_qkv, w_proj,
                norm0_a, conv0_a, norm0_b, conv0_b, upconv_0, norm1_a, conv1_a, norm1_b, conv1_b, upconv_1,
                norm2_a, conv2_a, norm2_b, conv2_b, skip_2, upconv_2, norm3_a, conv3_a, norm3_b, conv3_b,
                skip_3, norm_out, conv_out):
    n_col = net_shape[1]
    trows, tok_w, d = tokens.shape
    full = mlp(tokens.reshape(-1, d), tok_w, mod_vec, w_fc1, w_fc2, w_final, net_shape, 1)
    h, wid = 2 * trows, 2 * tok_w
    f, tot = attention(full.reshape(-1, full.shape[-1]), conv_in, norm_attn, w_qkv, w_proj, net_shape, 2)
    u = f.reshape(-1, f.shape[-1])
    blocks = [(norm0_a, conv0_a, norm0_b, conv0_b, (), upconv_0, h, h + 2, h + 1),
              (norm1_a, conv1_a, norm1_b, conv1_b, (), upconv_1, 16, 11, 13),
              (norm2_a, conv2_a, norm2_b, conv2_b, (skip_2,), upconv_2, 8, 10, 10),
              (norm3_a, conv3_a, norm3_b, conv3_b, (skip_3,), None, 8, 16, 0)]
    cid = 3
    for norm_a, conv_a, norm_b, conv_b, skip, up, blk_a, blk_b, blk_up in blocks:
        last = up is None
        g, tot = conv(u, tot, norm_a, conv_a, h, wid, net_shape, blk_a, 0, True, 2, last, cid)
        f, *tot = conv(g, tot, norm_b, conv_b, h, wid, net_shape, blk_b, 1, last, 0, last, cid + 1, u, *skip)
        if not last:
            u, tot = upconv(f, up, h, wid, net_shape, blk_up, cid + 2)
            h, wid = 2 * h, 2 * wid
        cid += 3
    tile = last_conv(f, tot[0], norm_out, conv_out, h, wid, net_shape, 16, cid)
    tile = tile.reshape(n_col, -1, h, wid // n_col).transpose(0, 2, 3, 1)
    return tile.reshape(n_col * h, wid // n_col, -1)


def solution(mesh):
    body_fn = functools.partial(device_body, (mesh.shape['row'], mesh.shape['col']))
    tok_spec = P(('batch', 'row', 'col'), None, None)
    out_spec = P(('batch', 'row'), 'col', None)
    return jax.shard_map(body_fn, mesh=mesh, in_specs=(tok_spec,) + (P(),) * 31, out_specs=out_spec, check_vma=False)
```

```python
import functools
import jax
import jax.numpy as jnp
from jax import lax
from jax.experimental import pallas as pl
from jax.experimental.pallas import tpu as pltpu
from jax.sharding import PartitionSpec as P

GROUPS = 32
LOG2_E = 1.4426950408889634
LANES = 128
SUB = 8
BASE = 16
F32, BF16 = jnp.float32, jnp.bfloat16
MESH = pl.DeviceIdType.MESH
VMEM_SPEC = pl.BlockSpec(memory_space=pltpu.VMEM)
MIB = 1 << 20
TOTALS = jax.ShapeDtypeStruct((1, LANES), F32)


def dot(a, b):
    return jnp.dot(a, b, preferred_element_type=F32)


def dot_t(a, b):
    return lax.dot_general(a, b, (((1,), (1,)), ((), ())), preferred_element_type=F32)


def exact_dot(a, b):
    return jnp.dot(a, b, preferred_element_type=F32, precision=lax.Precision.HIGHEST)


def clear(*refs):
    for ref in refs:
        ref[...] = jnp.zeros_like(ref)


def repeat(count, step):
    lax.fori_loop(0, count, step, 0)


def iota(shape, dim):
    return lax.broadcasted_iota(jnp.int32, shape, dim)


def aligned(first, size, unit):
    return pl.ds(pl.multiple_of(first, unit), size)


def layer_norm(v):
    mean = jnp.mean(v, axis=-1, keepdims=True)
    var = jnp.mean(jnp.square(v - mean), axis=-1, keepdims=True)
    return (v - mean) * lax.rsqrt(var + 1e-6)


def silu_of_half(half):
    return half + half * jnp.tanh(half)


class Net:
    def __init__(self, n_row, n_col):
        self.n_row, self.n_col = n_row, n_col
        self.n = n_row * n_col
        self.row, self.col = lax.axis_index('row'), lax.axis_index('col')
        self.strip = self.row * n_col + self.col

    def for_others(self, act, row_step=1):
        cols = [lax.rem(self.col + k, self.n_col) for k in range(self.n_col)]
        n_row = self.n_row // row_step

        def step(k, carry):
            row = lax.rem(self.row + (1 + lax.rem(k + n_row // 2 - 1, n_row - 1)) * row_step, self.n_row)
            for col in cols:
                act({'row': row, 'col': col})
            return carry
        repeat(n_row - 1, step)
        for col in cols[1:]:
            act({'row': self.row, 'col': col})
        return self.n // row_step - 1

    def beside(self, ahead):
        other = lax.rem(self.strip + ahead, self.n)
        return {'row': other // self.n_col, 'col': lax.rem(other, self.n_col)}

    def greet(self):
        barrier = pltpu.get_barrier_semaphore()
        self.for_others(lambda device: pl.semaphore_signal(barrier, inc=1, device_id=device, device_id_type=MESH))

    def all_here(self):
        pl.semaphore_wait(pltpu.get_barrier_semaphore(), self.n - 1)

    def to_others(self, src, recv, sems, row_step=1):
        count = self.for_others(lambda device: send(src, recv.at[self.strip], sems, device).start(), row_step)

        def wait():
            done = recv.at[pl.ds(0, count)]
            for side in range(2):
                pltpu.make_async_copy(done, done, sems.at[side]).wait()
        return wait


def send(src, dst, sems, device):
    return pltpu.make_async_remote_copy(
        src_ref=src, dst_ref=dst, send_sem=sems.at[0], recv_sem=sems.at[1], device_id=device, device_id_type=MESH)


PAIR_SEM = pltpu.SemaphoreType.DMA((2,))


def net_scratch(n, edge_shape=None):
    scratch = [pltpu.VMEM((1, LANES), F32), pltpu.VMEM((n, 1, LANES), F32), PAIR_SEM]
    if edge_shape is not None:
        scratch += [pltpu.VMEM((2,) + edge_shape, BF16), PAIR_SEM, PAIR_SEM]
    return scratch


def exchange(net, stat, stat_ref, recv, sems, tot_ref, sides=None, meanwhile=None):
    stat_ref[...] = stat
    net.all_here()
    wait = net.to_others(stat_ref, recv, sems)
    side_copies = []
    if sides is not None:
        first, last, top, bottom, hrecv, down_sems, up_sems = sides
        side_copies = [(send(src, hrecv.at[side], pair, net.beside(ahead)), dst, side) for side, (src, dst, pair, ahead)
                       in enumerate(((last, top, down_sems, 1), (first, bottom, up_sems, net.n - 1)))]
    for copy, _, _ in side_copies:
        copy.start()
    recv[net.strip] = stat
    if meanwhile:
        meanwhile()
    wait()
    tot_ref[...] = jnp.sum(recv[...], axis=0)
    for copy, dst, side in side_copies:
        copy.wait()
        dst[...] = hrecv[side]


def sum_scratch(ch):
    return [pltpu.VMEM((SUB, ch), F32)] * 2


def comm_params(cid, mib):
    return pltpu.CompilerParams(collective_id=cid, has_side_effects=True, vmem_limit_bytes=mib * MIB)


def mlp_kernel(net_shape, x_ref, mod_ref, w1_ref, w2_ref, wf_ref, o_ref,
               w1_buf, w2_buf, act_ref, acc_ref, part_ref, tok_ref, mix_ref, recv, w_sems, sems, swap_sems, pass_sems):
    net = Net(*net_shape)
    n_buf, blk = w1_buf.shape[0], w1_buf.shape[2]
    n_cut = w1_ref.shape[1] // blk // 2
    core = lax.rem(net.row, 2)
    partner = {'row': net.row + 1 - 2 * core, 'col': net.col}
    n_tok = x_ref.shape[0]

    def loads(i):
        part, slot = aligned((core * n_cut + i) * blk, blk, blk), lax.rem(i, n_buf)
        return [pltpu.make_async_copy(w1_ref.at[:, part], w1_buf.at[slot], w_sems.at[0, slot]),
                pltpu.make_async_copy(w2_ref.at[part], w2_buf.at[slot], w_sems.at[1, slot])]
    for i in range(n_cut):
        for load in loads(i):
            load.start()
    net.greet()
    shift1, scale1, gate1, shift2, scale2 = [mod_ref[pl.ds(i, 1)] for i in range(5)]
    x = x_ref[...].astype(F32)
    act = (layer_norm(x) * (1.0 + scale1) + shift1).astype(BF16)
    act_ref[0] = act
    clear(acc_ref)
    net.all_here()
    swap = send(act_ref.at[0], act_ref.at[1], swap_sems.at[0], partner)
    swap.start()
    swap.wait()

    def step(i, carry):
        load1, load2 = loads(i)
        slot = lax.rem(i, n_buf)
        load1.wait()
        hid = jax.nn.gelu(dot(act_ref[...].reshape(2 * n_tok, -1), w1_buf[slot]), approximate=True).astype(BF16)
        load2.wait()
        acc_ref[...] += dot(hid, w2_buf[slot]).reshape(acc_ref.shape)
        return carry
    repeat(n_cut, step)
    swap = send(acc_ref.at[1], part_ref, swap_sems.at[1], partner)
    swap.start()
    swap.wait()
    acc = acc_ref[0] + part_ref[...]
    y = (x + gate1 * acc).astype(BF16)
    fin = (layer_norm(y.astype(F32)) * (1.0 + scale2) + shift2).astype(BF16)
    tok_ref[...] = dot_t(fin, wf_ref[...])
    rows, part = mix_ref.shape[0] // 2, wf_ref.shape[0] // 2
    tok_w = tok_ref.shape[0] // rows
    toks = [tok_ref[pl.ds(j, rows, stride=tok_w), :] for j in range(tok_w)]
    for p in range(2):
        mix_ref[pl.ds(p, rows, stride=2), :] = jnp.concatenate([t[:, p * part:(p + 1) * part] for t in toks], axis=1)
    recv[net.strip] = mix_ref[...].astype(BF16)
    net.to_others(recv.at[net.strip], recv, sems, 2)()
    copies = []
    for i in range(net.n_row // 2):
        line = recv.at[pl.ds((2 * i + core) * net.n_col, net.n_col)]
        copies.append(send(line, line, pass_sems.at[i], partner))
        copies[-1].start()
    for copy in copies:
        copy.wait()
    o_ref[...] = recv[...]


def mlp(x, tok_w, mod_vec, w_fc1, w_fc2, w_final, net_shape, cid):
    n = net_shape[0] * net_shape[1]
    n_tok, d = x.shape
    hid, patch = w_fc1.shape[1], w_final.shape[1]
    n_buf = 4
    blk = hid // (2 * n_buf)
    rows = 2 * n_tok // tok_w
    lat = (rows, n_tok * patch // rows)
    hbm = pl.BlockSpec(memory_space=pltpu.HBM)
    return pl.pallas_call(
        functools.partial(mlp_kernel, net_shape),
        out_shape=jax.ShapeDtypeStruct((n,) + lat, BF16),
        in_specs=[VMEM_SPEC, VMEM_SPEC, hbm, hbm, VMEM_SPEC],
        out_specs=VMEM_SPEC,
        scratch_shapes=[pltpu.VMEM((n_buf, d, blk), BF16), pltpu.VMEM((n_buf, blk, d), BF16),
                        pltpu.VMEM((2,) + x.shape, BF16), pltpu.VMEM((2,) + x.shape, F32), pltpu.VMEM(x.shape, F32),
                        pltpu.VMEM((n_tok, patch), F32), pltpu.VMEM(lat, F32), pltpu.VMEM((n,) + lat, BF16),
                        pltpu.SemaphoreType.DMA((2, n_buf)), PAIR_SEM, pltpu.SemaphoreType.DMA((2, 2)), pltpu.SemaphoreType.DMA((net_shape[0] // 2, 2))],
        compiler_params=comm_params(cid, 48),
        name='mlp',
    )(x, mod_vec, w_fc1, w_fc2, w_final.T)


def in_group(channel, lane, per):
    return ((channel >= lane * per) & (channel < lane * per + per)).astype(F32)


def group_sums(s1, s2):
    ch = s1.shape[1]
    shape = (ch, LANES)
    both = [exact_dot(s, in_group(iota(shape, 0), iota(shape, 1) - at, ch // GROUPS))
            for s, at in ((s1, 0), (s2, GROUPS))]
    return jnp.sum(both[0] + both[1], axis=0, keepdims=True)


def norm_coefs(tot, norm_ref, ch, count):
    avg = jnp.broadcast_to(tot / count, (SUB, LANES))
    shape = (LANES, ch)
    mean, square = [exact_dot(avg, in_group(iota(shape, 1), iota(shape, 0) - at, ch // GROUPS)) for at in (0, GROUPS)]
    scale = lax.rsqrt(square - jnp.square(mean) + 1e-6) * norm_ref[0:1]
    return mean[0:1], scale[0:1], norm_ref[1:2]


def fold8(v):
    return jnp.sum(v.reshape(v.shape[0] // SUB, SUB, v.shape[1]), axis=0)


def attention_kernel(net_shape, lat_ref, win_ref, norm_ref, wqkv_ref, wproj_ref, out_ref, tot_ref,
                     cols_ref, toe_ref, fmap_ref, loc_ref, sc_ref, s1_ref, s2_ref, m_ref, l_ref, acc_ref,
                     stat_ref, recv, sems, *halo_refs):
    net = Net(*net_shape)
    net.greet()
    rows = lat_ref.shape[0]
    lat_c, ch = win_ref.shape[1:]
    wid = lat_ref.shape[1] // lat_c
    own = rows // net.n
    lat = lat_ref[...].astype(F32)
    idx = iota(lat.shape, 0)
    cols_ref[...] = jnp.concatenate([jnp.where(idx == 0, 0.0, pltpu.roll(lat, 1, 0)), lat,
                                     jnp.where(idx == rows - 1, 0.0, pltpu.roll(lat, rows - 1, 0))], axis=1).astype(BF16)
    clear(toe_ref)
    for x in range(wid):
        for tap in range(9):
            src = x + tap % 3 - 1
            if 0 <= src < wid:
                toe_ref[x, pl.ds(tap // 3 * LANES + src * lat_c, lat_c), :] = win_ref[tap]
    clear(s1_ref, s2_ref)
    blk = 1024
    per_col = rows // blk

    def conv_step(i, carry):
        y = dot(cols_ref[aligned(lax.rem(i, per_col) * blk, blk, blk), :], toe_ref[i // per_col]).astype(BF16)
        fmap_ref[aligned(i * blk, blk, blk), :] = y
        yf = y.astype(F32)
        s1_ref[...] += fold8(yf)
        s2_ref[...] += fold8(yf * yf)
        return carry
    repeat(wid * per_col, conv_step)
    mean, scale, shift = norm_coefs(group_sums(s1_ref[...], s2_ref[...]), norm_ref, ch, float(rows * wid * (ch // GROUPS)))

    for x in range(wid):
        loc_ref[x * own:(x + 1) * own, :] = fmap_ref[aligned(x * rows + net.strip * own, own, own), :]
    nl = ((loc_ref[...].astype(F32) - mean) * scale + shift).astype(BF16)
    q = dot(nl, wqkv_ref[:, :ch]).astype(BF16)
    qk = (dot_t(q, wqkv_ref[:, ch:2 * ch]) * (scale * (float(ch) ** -0.5 * LOG2_E))).astype(BF16)
    nk, n_q, kb = sc_ref.shape
    m_ref[...] = jnp.full_like(m_ref, -jnp.inf)

    def score_step(i, carry):
        s = dot_t(qk, fmap_ref[aligned(i * kb, kb, kb), :])
        sc_ref[i] = s
        m = m_ref[...]
        for j in range(kb // LANES):
            m = jnp.maximum(m, s[:, j * LANES:(j + 1) * LANES])
        m_ref[...] = m
        return carry
    repeat(nk, score_step)
    m_ref[...] = jnp.broadcast_to(jnp.max(m_ref[...], axis=1, keepdims=True), m_ref.shape)
    clear(l_ref, acc_ref)

    def value_step(i, carry):
        m = m_ref[...]
        tot_l = l_ref[...]
        parts = []
        for j in range(kb // LANES):
            e = jnp.exp2(sc_ref[i, :, j * LANES:(j + 1) * LANES] - m).astype(BF16)
            tot_l = tot_l + e.astype(F32)
            parts.append(e)
        l_ref[...] = tot_l
        acc_ref[...] += dot(jnp.concatenate(parts, axis=1), fmap_ref[aligned(i * kb, kb, kb), :])
        return carry
    repeat(nk, value_step)
    pn = acc_ref[...] / jnp.sum(l_ref[...], axis=1, keepdims=True)
    pn = ((pn - mean) * scale + shift).astype(BF16)
    att = dot(pn, wqkv_ref[:, 2 * ch:]).astype(BF16)
    out = (loc_ref[...].astype(F32) + dot(att, wproj_ref[...])).astype(BF16)
    i, j = iota((n_q, n_q), 0), iota((n_q, n_q), 1)
    perm = (j == lax.rem(i, wid) * own + i // wid).astype(BF16)
    of = dot(perm, out)
    out_ref[pl.ds(1, own)] = of.astype(BF16).reshape(own, wid, ch)
    exchange(net, group_sums(fold8(of), fold8(of * of)), stat_ref, recv, sems, tot_ref,
             (out_ref.at[1], out_ref.at[own], out_ref.at[0], out_ref.at[own + 1], *halo_refs))


def attention(lat, conv_in, norm, w_qkv, w_proj, net_shape, cid):
    n = net_shape[0] * net_shape[1]
    rows = lat.shape[0]
    lat_c, ch = conv_in.shape[2:]
    wid = lat.shape[1] // lat_c
    own = rows // n
    n_q = own * wid
    kb = 2048
    return pl.pallas_call(
        functools.partial(attention_kernel, net_shape),
        out_shape=[jax.ShapeDtypeStruct((own + 2, wid, ch), BF16), TOTALS],
        in_specs=[VMEM_SPEC] * 5, out_specs=[VMEM_SPEC] * 2,
        scratch_shapes=[pltpu.VMEM((rows, 3 * LANES), BF16), pltpu.VMEM((wid, 3 * LANES, ch), BF16),
                        pltpu.VMEM((rows * wid, ch), BF16), pltpu.VMEM((n_q, ch), BF16),
                        pltpu.VMEM((rows * wid // kb, n_q, kb), F32),
                        *sum_scratch(ch),
                        pltpu.VMEM((n_q, LANES), F32), pltpu.VMEM((n_q, LANES), F32), pltpu.VMEM((n_q, ch), F32)]
        + net_scratch(n, (wid, ch)),
        compiler_params=comm_params(cid, 27),
        name='attention',
    )(lat, conv_in.reshape(9, lat_c, ch), norm, w_qkv, w_proj)


def shifted(y, wid, by):
    n_px, ch = y.shape
    if wid > BASE:
        even, odd = jnp.split(y.reshape(n_px // wid, 2, wid // 2, ch), 2, axis=1)
        far = shifted((odd if by == 1 else even).reshape(n_px // 2, ch), wid // 2, by).reshape(even.shape)
        return jnp.concatenate([far, even] if by == 1 else [odd, far], axis=1).reshape(n_px, ch)
    tiles = pltpu.roll(y, by % n_px, 0).reshape(n_px // wid, wid // SUB, SUB, ch)
    at, sub = (0, 0) if by > 0 else (wid // SUB - 1, 7)
    edge = tiles[:, at:at + 1]
    edge = jnp.where(iota(edge.shape, 2) == sub, 0.0, edge)
    parts = [tiles[:, :at], edge, tiles[:, at + 1:]]
    return jnp.concatenate([p for p in parts if p.shape[1]], axis=1).reshape(n_px, ch)


class Rows:
    def __init__(self, net, x_ref, coefs, wid, h, pad, n_out, blk, pair):
        self.net, self.x_ref, self.coefs, self.wid, self.h, self.pad = net, x_ref, coefs, wid, h, pad
        self.n_out, self.blk, self.pair = n_out, blk, pair
        self.ch = x_ref.shape[-1]

    def inside(self, row):
        net = self.net
        return ((row >= self.pad) | (net.strip > 0)) & ((row < self.h + self.pad) | (net.strip < net.n - 1))

    def fill(self, buf, b, before=None):
        mean, scale, shift = self.coefs
        scale = 0.5 * scale
        shift = 0.5 * shift - mean * scale
        wid, ch, blk = self.wid, self.ch, self.blk
        if before is not None:
            self.keep_last(buf, before)
        together = -(-BASE // wid)
        for j in range(2 * (before is not None), blk + 2, together):
            row = b * blk + j
            if self.n_out > blk:
                row = jnp.minimum(row, self.n_out + 1)
            v = self.x_ref[aligned(row * wid, together * wid, SUB), :].astype(F32)
            if together == 1:
                keep = jnp.where(self.inside(row), 1.0, 0.0)
                y = silu_of_half(v * (scale * keep) + shift * keep)
            else:
                y = silu_of_half(v * scale + shift)
                y = jnp.where(self.inside(row + iota(y.shape, 0) // wid), y, 0.0)
            for lane, part in enumerate((shifted(y, wid, 1), y, shifted(y, wid, -1))):
                lanes = slice(lane * ch, (lane + 1) * ch)
                self.put(buf, j, together, lanes, part.astype(buf.dtype))

    def keep_last(self, buf, before):
        wid, blk = self.wid, self.blk
        if self.pair:
            buf[:, :wid, :] = before[:, blk // 2 * wid:, :]
        else:
            buf[:2 * wid, :] = before[blk * wid:, :]

    def put(self, buf, j, together, lanes, part):
        wid = self.wid
        if self.pair:
            buf[j % 2, j // 2 * wid:(j // 2 + 1) * wid, lanes] = part
        else:
            buf[j * wid:(j + together) * wid, lanes] = part

    def buffer(self):
        n_px, ch = (self.blk + 2) * self.wid, self.ch
        shape = (2, n_px // 2, 3 * ch) if self.pair else (n_px, 3 * ch)
        return pltpu.VMEM(shape, F32 if self.wid < 16 else BF16)

    def product(self, buf, w_ref):
        m = self.blk * self.wid // (2 if self.pair else 1)
        if self.pair:
            lhs = jnp.concatenate([buf[t % 2, t // 2 * self.wid:t // 2 * self.wid + m, :] for t in range(4)], axis=1)
            return dot(lhs, w_ref[...])
        acc = None
        for t in range(3):
            part = dot(buf[t * self.wid:t * self.wid + m, :].astype(BF16), w_ref[t])
            acc = part if acc is None else acc + part
        return acc

    def run(self, bufs, work):
        n_blk = -(-self.n_out // self.blk)
        self.fill(bufs[0], 0)
        if n_blk > 1:
            def step(i, carry):
                self.fill(bufs[1], 2 * i + 1, bufs[0])
                work(bufs[0], 2 * i)
                self.fill(bufs[0], 2 * i + 2, bufs[1])
                work(bufs[1], 2 * i + 1)
                return carry
            repeat(n_blk // 2, step)
        if n_blk % 2:
            work(bufs[0], n_blk - 1)


def paired_weights(w_ref, wp_ref):
    oc = w_ref.shape[2]
    clear(wp_ref)
    k = w_ref.shape[1]
    for t in range(3):
        wp_ref[t * k:(t + 1) * k, :oc] = w_ref[t]
        wp_ref[(t + 1) * k:(t + 2) * k, oc:] = w_ref[t]


def conv_kernel(cfg, *refs):
    net_shape, wid, h, blk, out_ext, pair, shortcut, stats, edge, skip_blk = cfg
    refs = iter(refs)
    x_ref, norm_tot_ref, norm_ref, w_ref = [next(refs) for _ in 'abcd']
    short_ref = next(refs) if shortcut else None
    skip_ref = next(refs) if skip_blk else None
    out_ref = next(refs)
    tot_ref = next(refs) if stats else None
    skip_out_ref = next(refs) if skip_blk else None
    buf0, buf1, s1_ref, s2_ref = [next(refs) for _ in 'abcd']
    wp_ref = next(refs) if pair else w_ref
    net_refs = list(refs)
    net = Net(*net_shape)
    if stats:
        net.greet()
    ch, oc = x_ref.shape[-1], w_ref.shape[2]
    n_out = h + 2 * out_ext
    coefs = norm_coefs(norm_tot_ref[...], norm_ref, ch, float(net.n * h * wid * (ch // GROUPS)))
    rows = Rows(net, x_ref, coefs, wid, h, 1 + out_ext, n_out, blk, pair)
    clear(s1_ref, s2_ref)
    if pair:
        paired_weights(w_ref, wp_ref)
    exact = n_out % blk == 0 and not out_ext

    def count(y, first_row, step):
        yf = y.astype(F32)
        if exact:
            s1_ref[...] += fold8(yf)
            s2_ref[...] += fold8(yf * yf)
            return
        for i, part in enumerate(jnp.split(yf, yf.shape[0] // wid)):
            r = first_row + step * i
            own = (r >= out_ext) & (r < h + out_ext)
            s1_ref[...] += jnp.where(own, fold8(part), 0.0)
            s2_ref[...] += jnp.where(own, fold8(part * part), 0.0)

    def work(buf, b):
        k0 = b * blk
        acc = rows.product(buf, wp_ref)
        if pair:
            for a in range(2):
                val = acc[:, a * oc:(a + 1) * oc]
                here = pl.ds(edge // 2 + k0 // 2, blk // 2)
                if shortcut:
                    val = short_ref[pl.ds(k0 // 2, blk // 2), a].reshape(val.shape) + val
                y = val.astype(BF16)
                out_ref[here, a] = y.reshape(blk // 2, wid, oc)
                if stats:
                    count(y, k0 + a, 2)
        else:
            if shortcut:
                acc = short_ref[aligned(k0 * wid, blk * wid, SUB), :].astype(F32) + acc
            y = acc.astype(BF16)
            out_ref[aligned((k0 + edge) * wid, blk * wid, SUB), :] = y
            if stats:
                count(y, k0, 1)
    rows.run((buf0, buf1), work)
    if out_ext:
        for at, at_edge in ((0, net.strip == 0), (n_out - 1, net.strip == net.n - 1)):
            where = out_ref.at[at // 2, at % 2] if pair else out_ref.at[pl.ds(at * wid, wid)]

            @pl.when(at_edge)
            def _():
                where[...] = jnp.zeros(where.shape, BF16)
    if stats:
        sides = None
        if edge:
            def part(row):
                return out_ref.at[row // 2] if pair else out_ref.at[pl.ds(row * wid, edge * wid)]
            sides = (part(edge), part(h), part(0), part(h + edge), *net_refs[3:])

        def skip_step(b, carry):
            here = aligned(b * skip_blk * wid, skip_blk * wid, SUB)
            skip_out_ref[here, :] = dot(x_ref[here, :], skip_ref[...])
            return carry

        def skip_all():
            repeat(skip_out_ref.shape[0] // (skip_blk * wid), skip_step)
        exchange(net, group_sums(s1_ref[...], s2_ref[...]), *net_refs[:3], tot_ref, sides, skip_all if skip_blk else None)


def conv(x, tot, norm, w, h, wid, net_shape, blk, out_ext, stats, edge, pair, cid, short, skip):
    n = net_shape[0] * net_shape[1]
    ch, oc = w.shape[2:]
    args = [x, tot, norm, w.reshape(3, 3 * ch, oc)]
    for src in short:
        args.append(src.reshape(-1, 2, wid, src.shape[-1]) if pair else src)
    args += skip[:1]
    n_out = h + 2 * out_ext
    rows = -(-n_out // blk) * blk + 2 * edge
    outs = [jax.ShapeDtypeStruct((rows // 2, 2, wid, oc) if pair else (rows * wid, oc), BF16)]
    if stats:
        outs.append(TOTALS)
    cfg = (net_shape, wid, h, blk, out_ext, pair, bool(short), stats, edge, skip[1] if skip else 0)
    if skip:
        outs.append(jax.ShapeDtypeStruct((skip[2] * wid, skip[0].shape[1]), F32))
    layout = Rows(None, x, None, wid, h, None, n_out, blk, pair)
    scratch = [layout.buffer(), layout.buffer(), *sum_scratch(oc)]
    if pair:
        scratch.append(pltpu.VMEM((12 * ch, 2 * oc), BF16))
    if stats:
        scratch += net_scratch(n, ((2, wid, oc) if pair else (edge * wid, oc)) if edge else None)
    px = n_out * wid
    res = pl.pallas_call(
        functools.partial(conv_kernel, cfg),
        out_shape=outs, in_specs=[VMEM_SPEC] * len(args), out_specs=[VMEM_SPEC] * len(outs),
        scratch_shapes=scratch,
        compiler_params=comm_params(cid, 28) if stats else pltpu.CompilerParams(vmem_limit_bytes=28 * MIB),
        cost_estimate=pl.CostEstimate(flops=18 * ch * oc * px, bytes_accessed=2 * px * (ch + oc), transcendentals=px * ch),
        name='conv_w%d_%d_%d' % (wid, ch, oc) + ('e' if out_ext else ''),
    )(*args)
    return [res[0].reshape(rows * wid, oc)] + list(res[1:])


def upconv_kernel(cfg, x_ref, w_ref, out_ref, tot_ref, s1_ref, s2_ref, mix_ref, stat_ref, recv, sems):
    net_shape, half, hs, blk = cfg
    net = Net(*net_shape)
    net.greet()
    oc = w_ref.shape[2]
    n_k = hs + 1
    mixed = half < BASE
    m, more = blk * half, (blk + 1) * half
    clear(s1_ref, s2_ref)

    def step(b, carry):
        k0 = jnp.minimum(b * blk, n_k - blk) if n_k > blk else 0
        x = x_ref[aligned(k0 * half, more, SUB), :]
        rows = []
        for dx in range(3):
            above, mid, below = [dot(x, w_ref[3 * dy + dx]) for dy in range(3)]
            both = above[:m] + below[half:]
            rows.append((both + mid[:m], both + mid[half:]))
        for a in range(2):
            left, at, right = [r[a] for r in rows]
            even = at + right + shifted(left, half, 1)
            odd = left + at + shifted(right, half, -1)
            for q, val in ((0, even), (1, odd)):
                y = val.astype(BF16)
                if mixed:
                    for c in range(0, oc, LANES):
                        mix_ref[a, c // LANES, pl.ds(q, m, stride=2), :] = val[:, c:c + LANES]
                else:
                    out_ref[pl.ds(k0, blk), a, q * half:(q + 1) * half, :] = y.reshape(blk, half, oc)
                yf = y.astype(F32)
                for i, part in enumerate(jnp.split(yf, blk)):
                    k = k0 + i
                    own = (k >= b * blk) & ((k < hs) if a else (k > 0))
                    s1_ref[...] += jnp.where(own, fold8(part), 0.0)
                    s2_ref[...] += jnp.where(own, fold8(part * part), 0.0)
            for c in range(0, oc if mixed else 0, LANES):
                out_ref[pl.ds(k0, blk), a, :, c:c + LANES] = mix_ref[a, c // LANES].astype(BF16).reshape(blk, 2 * half, LANES)
        return carry
    if n_k == blk:
        step(0, 0)
    else:
        repeat(-(-n_k // blk), step)
    exchange(net, group_sums(s1_ref[...], s2_ref[...]), stat_ref, recv, sems, tot_ref)


def upconv(x, w, hs, half, net_shape, blk, cid):
    n = net_shape[0] * net_shape[1]
    ch, oc = w.shape[2:]
    n_k = hs + 8
    px = 4 * n_k * half
    out, tot = pl.pallas_call(
        functools.partial(upconv_kernel, (net_shape, half, hs, blk)),
        out_shape=[jax.ShapeDtypeStruct((n_k, 2, 2 * half, oc), BF16), TOTALS],
        in_specs=[VMEM_SPEC] * 2, out_specs=[VMEM_SPEC] * 2,
        scratch_shapes=[*sum_scratch(oc),
                        pltpu.VMEM((2, oc // LANES, 2 * blk * half if half < BASE else SUB, LANES), F32)] + net_scratch(n),
        compiler_params=comm_params(cid, 28),
        cost_estimate=pl.CostEstimate(flops=5 * ch * oc * px, bytes_accessed=2 * px * (ch + oc), transcendentals=0),
        name='upconv_w%d' % (2 * half),
    )(x, w.reshape(9, ch, oc))
    return out.reshape(px, oc), tot


class QuarterRows(Rows):
    def keep_last(self, buf, before):
        buf[:, :2 * self.tile] = before[:, self.blk * self.tile:]

    def put(self, buf, j, together, lanes, part):
        n_q = buf.shape[0]
        here = self.tile // (self.wid // BASE)
        whole = part.reshape(self.wid // BASE, BASE, part.shape[1])
        for q in range(n_q):
            buf[q, j * self.tile:(j + 1) * self.tile, lanes] = whole[:, q * here:(q + 1) * here].reshape(self.tile, part.shape[1])


def last_kernel(cfg, x_ref, tot_ref, norm_ref, w_ref, out_ref, buf0, buf1, mine, recv, send_sems, recv_sems):
    net_shape, wid, h, blk, oc = cfg
    net = Net(*net_shape)
    barrier = pltpu.get_barrier_semaphore()
    cols = [lax.rem(net.col + k, net.n_col) for k in range(net.n_col)]
    for col in cols[1:]:
        pl.semaphore_signal(barrier, inc=1, device_id={'col': col}, device_id_type=MESH)
    ch = x_ref.shape[1]
    coefs = norm_coefs(tot_ref[...], norm_ref, ch, float(net.n * h * wid * (ch // GROUPS)))
    rows = QuarterRows(net, x_ref, coefs, wid, h, 1, h, blk, False)
    rows.tile = tile = wid // net.n_col
    m = blk * tile
    per = h * tile // LANES

    def work(buf, b):
        for q in range(net.n_col):
            z = dot_t(w_ref[...], buf[q])
            z = z[:SUB, :m] + z[SUB:16, tile:tile + m] + z[16:, 2 * tile:2 * tile + m]
            for c in range(oc):
                for t in range(m // LANES):
                    mine[q, pl.ds(c * per + b * (m // LANES) + t, 1), :] = z[c:c + 1, t * LANES:(t + 1) * LANES]
    rows.run((buf0, buf1), work)
    pl.semaphore_wait(barrier, net.n_col - 1)
    copies = []
    for k, col in enumerate(cols[1:]):
        copies.append(pltpu.make_async_remote_copy(
            src_ref=mine.at[col], dst_ref=recv.at[net.col], send_sem=send_sems.at[k], recv_sem=recv_sems.at[k],
            device_id={'col': col}, device_id_type=MESH))
        copies[-1].start()
    recv[net.col] = mine[net.col]
    for copy in copies:
        copy.wait()
    i, j = iota((LANES, LANES), 0), iota((LANES, LANES), 1)
    splits = wid // BASE
    lane, run = lax.rem(j, tile), j // tile
    src = run * tile + lax.rem(lane, 2) * (tile // 2) + lax.rem(lane // 2, splits // 2) * (tile // splits) + lane // splits
    perm = (i == src).astype(F32)
    for q in range(net.n_col):
        out_ref[q] = exact_dot(recv[q], perm)


def last_conv(x, tot, norm, w, h, wid, net_shape, blk, cid):
    n_col = net_shape[1]
    ch, oc = w.shape[2:]
    wt = jnp.zeros((3, SUB, 3 * ch), BF16).at[:, :oc].set(w.reshape(3, 3 * ch, oc).transpose(0, 2, 1))
    buf = pltpu.VMEM((n_col, (blk + 2) * wid // n_col, 3 * ch), BF16)
    shape = (n_col, oc * h * wid // n_col // LANES, LANES)
    return pl.pallas_call(
        functools.partial(last_kernel, (net_shape, wid, h, blk, oc)),
        out_shape=jax.ShapeDtypeStruct(shape, F32),
        in_specs=[VMEM_SPEC] * 4, out_specs=VMEM_SPEC,
        scratch_shapes=[buf, buf, pltpu.VMEM(shape, F32), pltpu.VMEM(shape, F32)] + [pltpu.SemaphoreType.DMA((n_col,))] * 2,
        compiler_params=comm_params(cid, 28),
        name='last_conv',
    )(x, tot, norm, wt.reshape(-1, 3 * ch))


def device_body(net_shape, tokens, mod_vec, w_fc1, w_fc2, w_final, conv_in, norm_attn, w_qkv, w_proj,
                norm0_a, conv0_a, norm0_b, conv0_b, upconv_0, norm1_a, conv1_a, norm1_b, conv1_b, upconv_1,
                norm2_a, conv2_a, norm2_b, conv2_b, skip_2, upconv_2, norm3_a, conv3_a, norm3_b, conv3_b,
                skip_3, norm_out, conv_out):
    n_col = net_shape[1]
    trows, tok_w, d = tokens.shape
    full = mlp(tokens.reshape(-1, d), tok_w, mod_vec, w_fc1, w_fc2, w_final, net_shape, 1)
    h, wid = 2 * trows, 2 * tok_w
    f, tot = attention(full.reshape(-1, full.shape[-1]), conv_in, norm_attn, w_qkv, w_proj, net_shape, 2)
    u = f.reshape(-1, f.shape[-1])
    blocks = [(norm0_a, conv0_a, norm0_b, conv0_b, (), upconv_0, h, h + 2, h + 1),
              (norm1_a, conv1_a, norm1_b, conv1_b, (), upconv_1, 16, 11, 13),
              (norm2_a, conv2_a, norm2_b, conv2_b, (skip_2,), upconv_2, 16, 10, 10),
              (norm3_a, conv3_a, norm3_b, conv3_b, (skip_3,), None, 16, 16, 0)]
    cid = 3
    for norm_a, conv_a, norm_b, conv_b, skip, up, blk_a, blk_b, blk_up in blocks:
        last = up is None
        skip = [(m, blk_b, -(-(h + 2) // blk_b) * blk_b) for m in skip]
        g, tot, *short = conv(u, tot, norm_a, conv_a, h, wid, net_shape, blk_a, 0, True, 2, last, cid, (), *skip or [()])
        f, *tot = conv(g, tot, norm_b, conv_b, h, wid, net_shape, blk_b, 1, last, 0, last, cid + 1, short or (u,), ())
        if not last:
            u, tot = upconv(f, up, h, wid, net_shape, blk_up, cid + 2)
            h, wid = 2 * h, 2 * wid
        cid += 3
    tile = last_conv(f, tot[0], norm_out, conv_out, h, wid, net_shape, 16, cid)
    tile = tile.reshape(n_col, -1, h, wid // n_col).transpose(0, 2, 3, 1)
    return tile.reshape(n_col * h, wid // n_col, -1)


def solution(mesh):
    body_fn = functools.partial(device_body, (mesh.shape['row'], mesh.shape['col']))
    tok_spec = P(('batch', 'row', 'col'), None, None)
    out_spec = P(('batch', 'row'), 'col', None)
    return jax.shard_map(body_fn, mesh=mesh, in_specs=(tok_spec,) + (P(),) * 31, out_specs=out_spec, check_vma=False)
```

```python
import functools
import jax
import jax.numpy as jnp
from jax import lax
from jax.experimental import pallas as pl
from jax.experimental.pallas import tpu as pltpu
from jax.sharding import PartitionSpec as P

GROUPS = 32
LOG2_E = 1.4426950408889634
LANES = 128
SUB = 8
BASE = 16
F32, BF16 = jnp.float32, jnp.bfloat16
MESH = pl.DeviceIdType.MESH
VMEM_SPEC = pl.BlockSpec(memory_space=pltpu.VMEM)
MIB = 1 << 20
TOTALS = jax.ShapeDtypeStruct((1, LANES), F32)


def dot(a, b):
    return jnp.dot(a, b, preferred_element_type=F32)


def dot_t(a, b):
    return lax.dot_general(a, b, (((1,), (1,)), ((), ())), preferred_element_type=F32)


def exact_dot(a, b):
    return jnp.dot(a, b, preferred_element_type=F32, precision=lax.Precision.HIGHEST)


def clear(*refs):
    for ref in refs:
        ref[...] = jnp.zeros_like(ref)


def repeat(count, step):
    lax.fori_loop(0, count, step, 0)


def iota(shape, dim):
    return lax.broadcasted_iota(jnp.int32, shape, dim)


def aligned(first, size, unit):
    return pl.ds(pl.multiple_of(first, unit), size)


def layer_norm(v):
    mean = jnp.mean(v, axis=-1, keepdims=True)
    var = jnp.mean(jnp.square(v - mean), axis=-1, keepdims=True)
    return (v - mean) * lax.rsqrt(var + 1e-6)


def silu_of_half(half):
    return half + half * jnp.tanh(half)


class Net:
    def __init__(self, n_row, n_col):
        self.n_row, self.n_col = n_row, n_col
        self.n = n_row * n_col
        self.row, self.col = lax.axis_index('row'), lax.axis_index('col')
        self.strip = self.row * n_col + self.col
        self.met = False

    def for_others(self, act, row_step=1):
        cols = [lax.rem(self.col + k, self.n_col) for k in range(self.n_col)]
        n_row = self.n_row // row_step

        def step(k, carry):
            row = lax.rem(self.row + (1 + lax.rem(k + n_row // 2 - 1, n_row - 1)) * row_step, self.n_row)
            for col in cols:
                act({'row': row, 'col': col})
            return carry
        repeat(n_row - 1, step)
        for col in cols[1:]:
            act({'row': self.row, 'col': col})
        return self.n // row_step - 1

    def beside(self, ahead):
        other = lax.rem(self.strip + ahead, self.n)
        return {'row': other // self.n_col, 'col': lax.rem(other, self.n_col)}

    def greet(self):
        barrier = pltpu.get_barrier_semaphore()
        self.for_others(lambda device: pl.semaphore_signal(barrier, inc=1, device_id=device, device_id_type=MESH))

    def all_here(self):
        if not self.met:
            pl.semaphore_wait(pltpu.get_barrier_semaphore(), self.n - 1)
        self.met = True

    def to_others(self, src, recv, sems, row_step=1):
        count = self.for_others(lambda device: send(src, recv.at[self.strip], sems, device).start(), row_step)

        def wait():
            done = recv.at[pl.ds(0, count)]
            for side in range(2):
                pltpu.make_async_copy(done, done, sems.at[side]).wait()
        return wait


def send(src, dst, sems, device):
    return pltpu.make_async_remote_copy(
        src_ref=src, dst_ref=dst, send_sem=sems.at[0], recv_sem=sems.at[1], device_id=device, device_id_type=MESH)


PAIR_SEM = pltpu.SemaphoreType.DMA((2,))


def net_scratch(n, edge_shape=None):
    scratch = [pltpu.VMEM((1, LANES), F32), pltpu.VMEM((n, 1, LANES), F32), PAIR_SEM]
    if edge_shape is not None:
        scratch += [pltpu.VMEM((2,) + edge_shape, BF16), PAIR_SEM, PAIR_SEM]
    return scratch


def exchange(net, stat, stat_ref, recv, sems, tot_ref, sides=None, meanwhile=None):
    stat_ref[...] = stat
    net.all_here()
    wait = net.to_others(stat_ref, recv, sems)
    side_copies = []
    if sides is not None:
        first, last, top, bottom, hrecv, down_sems, up_sems = sides
        side_copies = [(send(src, hrecv.at[side], pair, net.beside(ahead)), dst, side) for side, (src, dst, pair, ahead)
                       in enumerate(((last, top, down_sems, 1), (first, bottom, up_sems, net.n - 1)))]
    for copy, _, _ in side_copies:
        copy.start()
    recv[net.strip] = stat
    if meanwhile:
        meanwhile()
    wait()
    tot_ref[...] = jnp.sum(recv[...], axis=0)
    for copy, dst, side in side_copies:
        copy.wait()
        dst[...] = hrecv[side]


def sum_scratch(ch):
    return [pltpu.VMEM((SUB, ch), F32)] * 2


def comm_params(cid, mib):
    return pltpu.CompilerParams(collective_id=cid, has_side_effects=True, vmem_limit_bytes=mib * MIB)


def mlp_kernel(net_shape, x_ref, mod_ref, w1_ref, w2_ref, wf_ref, o_ref,
               w1_buf, w2_buf, act_ref, acc_ref, part_ref, tok_ref, mix_ref, recv, w_sems, sems, swap_sems, pass_sems):
    net = Net(*net_shape)
    n_buf, blk = w1_buf.shape[0], w1_buf.shape[2]
    n_cut = w1_ref.shape[1] // blk // 2
    core = lax.rem(net.row, 2)
    partner = {'row': net.row + 1 - 2 * core, 'col': net.col}
    n_tok = x_ref.shape[0]

    def loads(i):
        part, slot = aligned((core * n_cut + i) * blk, blk, blk), lax.rem(i, n_buf)
        return [pltpu.make_async_copy(w1_ref.at[:, part], w1_buf.at[slot], w_sems.at[0, slot]),
                pltpu.make_async_copy(w2_ref.at[part], w2_buf.at[slot], w_sems.at[1, slot])]
    for i in range(n_cut):
        for load in loads(i):
            load.start()
    net.greet()
    shift1, scale1, gate1, shift2, scale2 = [mod_ref[pl.ds(i, 1)] for i in range(5)]
    x = x_ref[...].astype(F32)
    act = (layer_norm(x) * (1.0 + scale1) + shift1).astype(BF16)
    act_ref[0] = act
    clear(acc_ref)
    net.all_here()
    swap = send(act_ref.at[0], act_ref.at[1], swap_sems.at[0], partner)
    swap.start()
    swap.wait()

    def step(i, carry):
        load1, load2 = loads(i)
        slot = lax.rem(i, n_buf)
        load1.wait()
        hid = jax.nn.gelu(dot(act_ref[...].reshape(2 * n_tok, -1), w1_buf[slot]), approximate=True).astype(BF16)
        load2.wait()
        acc_ref[...] += dot(hid, w2_buf[slot]).reshape(acc_ref.shape)
        return carry
    repeat(n_cut, step)
    swap = send(acc_ref.at[1], part_ref, swap_sems.at[1], partner)
    swap.start()
    swap.wait()
    acc = acc_ref[0] + part_ref[...]
    y = (x + gate1 * acc).astype(BF16)
    fin = (layer_norm(y.astype(F32)) * (1.0 + scale2) + shift2).astype(BF16)
    tok_ref[...] = dot_t(fin, wf_ref[...])
    rows, part = mix_ref.shape[0] // 2, wf_ref.shape[0] // 2
    tok_w = tok_ref.shape[0] // rows
    toks = [tok_ref[pl.ds(j, rows, stride=tok_w), :] for j in range(tok_w)]
    for p in range(2):
        mix_ref[pl.ds(p, rows, stride=2), :] = jnp.concatenate([t[:, p * part:(p + 1) * part] for t in toks], axis=1)
    recv[net.strip] = mix_ref[...].astype(BF16)
    net.to_others(recv.at[net.strip], recv, sems, 2)()
    copies = []
    for i in range(net.n_row // 2):
        line = recv.at[pl.ds((2 * i + core) * net.n_col, net.n_col)]
        copies.append(send(line, line, pass_sems.at[i], partner))
        copies[-1].start()
    for copy in copies:
        copy.wait()
    o_ref[...] = recv[...]


def mlp(x, tok_w, mod_vec, w_fc1, w_fc2, w_final, net_shape, cid):
    n = net_shape[0] * net_shape[1]
    n_tok, d = x.shape
    hid, patch = w_fc1.shape[1], w_final.shape[1]
    n_buf = 4
    blk = hid // (2 * n_buf)
    rows = 2 * n_tok // tok_w
    lat = (rows, n_tok * patch // rows)
    hbm = pl.BlockSpec(memory_space=pltpu.HBM)
    return pl.pallas_call(
        functools.partial(mlp_kernel, net_shape),
        out_shape=jax.ShapeDtypeStruct((n,) + lat, BF16),
        in_specs=[VMEM_SPEC, VMEM_SPEC, hbm, hbm, VMEM_SPEC],
        out_specs=VMEM_SPEC,
        scratch_shapes=[pltpu.VMEM((n_buf, d, blk), BF16), pltpu.VMEM((n_buf, blk, d), BF16),
                        pltpu.VMEM((2,) + x.shape, BF16), pltpu.VMEM((2,) + x.shape, F32), pltpu.VMEM(x.shape, F32),
                        pltpu.VMEM((n_tok, patch), F32), pltpu.VMEM(lat, F32), pltpu.VMEM((n,) + lat, BF16),
                        pltpu.SemaphoreType.DMA((2, n_buf)), PAIR_SEM, pltpu.SemaphoreType.DMA((2, 2)), pltpu.SemaphoreType.DMA((net_shape[0] // 2, 2))],
        compiler_params=comm_params(cid, 46),
        name='mlp',
    )(x, mod_vec, w_fc1, w_fc2, w_final.T)


def in_group(channel, lane, per):
    return ((channel >= lane * per) & (channel < lane * per + per)).astype(F32)


def group_sums(s1, s2):
    ch = s1.shape[1]
    shape = (ch, LANES)
    both = [exact_dot(s, in_group(iota(shape, 0), iota(shape, 1) - at, ch // GROUPS))
            for s, at in ((s1, 0), (s2, GROUPS))]
    return jnp.sum(both[0] + both[1], axis=0, keepdims=True)


def norm_coefs(tot, norm_ref, ch, count):
    avg = jnp.broadcast_to(tot / count, (SUB, LANES))
    shape = (LANES, ch)
    mean, square = [exact_dot(avg, in_group(iota(shape, 1), iota(shape, 0) - at, ch // GROUPS)) for at in (0, GROUPS)]
    scale = lax.rsqrt(square - jnp.square(mean) + 1e-6) * norm_ref[0:1]
    return mean[0:1], scale[0:1], norm_ref[1:2]


def fold8(v):
    return jnp.sum(v.reshape(v.shape[0] // SUB, SUB, v.shape[1]), axis=0)


def attention_kernel(net_shape, lat_ref, win_ref, norm_ref, wqkv_ref, wproj_ref, out_ref, tot_ref,
                     cols_ref, toe_ref, fmap_ref, loc_ref, sc_ref, s1_ref, s2_ref, m_ref, l_ref, acc_ref,
                     stat_ref, recv, sems, *halo_refs):
    net = Net(*net_shape)
    net.greet()
    rows = lat_ref.shape[0]
    lat_c, ch = win_ref.shape[1:]
    wid = lat_ref.shape[1] // lat_c
    own = rows // net.n
    lat = lat_ref[...].astype(F32)
    idx = iota(lat.shape, 0)
    cols_ref[...] = jnp.concatenate([jnp.where(idx == 0, 0.0, pltpu.roll(lat, 1, 0)), lat,
                                     jnp.where(idx == rows - 1, 0.0, pltpu.roll(lat, rows - 1, 0))], axis=1).astype(BF16)
    clear(toe_ref)
    for x in range(wid):
        for tap in range(9):
            src = x + tap % 3 - 1
            if 0 <= src < wid:
                toe_ref[x, pl.ds(tap // 3 * LANES + src * lat_c, lat_c), :] = win_ref[tap]
    clear(s1_ref, s2_ref)
    blk = 1024
    per_col = rows // blk

    def conv_step(i, carry):
        y = dot(cols_ref[aligned(lax.rem(i, per_col) * blk, blk, blk), :], toe_ref[i // per_col]).astype(BF16)
        fmap_ref[aligned(i * blk, blk, blk), :] = y
        yf = y.astype(F32)
        s1_ref[...] += fold8(yf)
        s2_ref[...] += fold8(yf * yf)
        return carry
    repeat(wid * per_col, conv_step)
    mean, scale, shift = norm_coefs(group_sums(s1_ref[...], s2_ref[...]), norm_ref, ch, float(rows * wid * (ch // GROUPS)))

    for x in range(wid):
        loc_ref[x * own:(x + 1) * own, :] = fmap_ref[aligned(x * rows + net.strip * own, own, own), :]
    nl = ((loc_ref[...].astype(F32) - mean) * scale + shift).astype(BF16)
    q = dot(nl, wqkv_ref[:, :ch]).astype(BF16)
    qk = (dot_t(q, wqkv_ref[:, ch:2 * ch]) * (scale * (float(ch) ** -0.5 * LOG2_E))).astype(BF16)
    nk, n_q, kb = sc_ref.shape
    m_ref[...] = jnp.full_like(m_ref, -jnp.inf)

    def score_step(i, carry):
        s = dot_t(qk, fmap_ref[aligned(i * kb, kb, kb), :])
        sc_ref[i] = s
        m = m_ref[...]
        for j in range(kb // LANES):
            m = jnp.maximum(m, s[:, j * LANES:(j + 1) * LANES])
        m_ref[...] = m
        return carry
    repeat(nk, score_step)
    m_ref[...] = jnp.broadcast_to(jnp.max(m_ref[...], axis=1, keepdims=True), m_ref.shape)
    clear(l_ref, acc_ref)

    def value_step(i, carry):
        m = m_ref[...]
        tot_l = l_ref[...]
        parts = []
        for j in range(kb // LANES):
            e = jnp.exp2(sc_ref[i, :, j * LANES:(j + 1) * LANES] - m).astype(BF16)
            tot_l = tot_l + e.astype(F32)
            parts.append(e)
        l_ref[...] = tot_l
        acc_ref[...] += dot(jnp.concatenate(parts, axis=1), fmap_ref[aligned(i * kb, kb, kb), :])
        return carry
    repeat(nk, value_step)
    pn = acc_ref[...] / jnp.sum(l_ref[...], axis=1, keepdims=True)
    pn = ((pn - mean) * scale + shift).astype(BF16)
    att = dot(pn, wqkv_ref[:, 2 * ch:]).astype(BF16)
    out = (loc_ref[...].astype(F32) + dot(att, wproj_ref[...])).astype(BF16)
    i, j = iota((n_q, n_q), 0), iota((n_q, n_q), 1)
    perm = (j == lax.rem(i, wid) * own + i // wid).astype(BF16)
    of = dot(perm, out)
    out_ref[pl.ds(1, own)] = of.astype(BF16).reshape(own, wid, ch)
    exchange(net, group_sums(fold8(of), fold8(of * of)), stat_ref, recv, sems, tot_ref,
             (out_ref.at[1], out_ref.at[own], out_ref.at[0], out_ref.at[own + 1], *halo_refs))


def attention(lat, conv_in, norm, w_qkv, w_proj, net_shape, cid):
    n = net_shape[0] * net_shape[1]
    rows = lat.shape[0]
    lat_c, ch = conv_in.shape[2:]
    wid = lat.shape[1] // lat_c
    own = rows // n
    n_q = own * wid
    kb = 2048
    return pl.pallas_call(
        functools.partial(attention_kernel, net_shape),
        out_shape=[jax.ShapeDtypeStruct((own + 2, wid, ch), BF16), TOTALS],
        in_specs=[VMEM_SPEC] * 5, out_specs=[VMEM_SPEC] * 2,
        scratch_shapes=[pltpu.VMEM((rows, 3 * LANES), BF16), pltpu.VMEM((wid, 3 * LANES, ch), BF16),
                        pltpu.VMEM((rows * wid, ch), BF16), pltpu.VMEM((n_q, ch), BF16),
                        pltpu.VMEM((rows * wid // kb, n_q, kb), F32),
                        *sum_scratch(ch),
                        pltpu.VMEM((n_q, LANES), F32), pltpu.VMEM((n_q, LANES), F32), pltpu.VMEM((n_q, ch), F32)]
        + net_scratch(n, (wid, ch)),
        compiler_params=comm_params(cid, 27),
        name='attention',
    )(lat, conv_in.reshape(9, lat_c, ch), norm, w_qkv, w_proj)


def shifted(y, wid, by):
    n_px, ch = y.shape
    if wid > BASE:
        even, odd = jnp.split(y.reshape(n_px // wid, 2, wid // 2, ch), 2, axis=1)
        far = shifted((odd if by == 1 else even).reshape(n_px // 2, ch), wid // 2, by).reshape(even.shape)
        return jnp.concatenate([far, even] if by == 1 else [odd, far], axis=1).reshape(n_px, ch)
    tiles = pltpu.roll(y, by % n_px, 0).reshape(n_px // wid, wid // SUB, SUB, ch)
    at, sub = (0, 0) if by > 0 else (wid // SUB - 1, 7)
    edge = tiles[:, at:at + 1]
    edge = jnp.where(iota(edge.shape, 2) == sub, 0.0, edge)
    parts = [tiles[:, :at], edge, tiles[:, at + 1:]]
    return jnp.concatenate([p for p in parts if p.shape[1]], axis=1).reshape(n_px, ch)


class Rows:
    def __init__(self, net, x_ref, coefs, wid, h, pad, n_out, blk, pair):
        self.net, self.x_ref, self.coefs, self.wid, self.h, self.pad = net, x_ref, coefs, wid, h, pad
        self.n_out, self.blk, self.pair = n_out, blk, pair
        self.ch = x_ref.shape[-1]

    def inside(self, row):
        net = self.net
        return ((row >= self.pad) | (net.strip > 0)) & ((row < self.h + self.pad) | (net.strip < net.n - 1))

    def fill(self, buf, b, before=None):
        mean, scale, shift = self.coefs
        scale = 0.5 * scale
        shift = 0.5 * shift - mean * scale
        wid, ch, blk = self.wid, self.ch, self.blk
        if before is not None:
            self.keep_last(buf, before)
        together = -(-BASE // wid)
        for j in range(2 * (before is not None), blk + 2, together):
            row = b * blk + j
            if self.n_out > blk:
                row = jnp.minimum(row, self.n_out + 1)
            v = self.x_ref[aligned(row * wid, together * wid, SUB), :].astype(F32)
            if together == 1:
                keep = jnp.where(self.inside(row), 1.0, 0.0)
                y = silu_of_half(v * (scale * keep) + shift * keep)
            else:
                y = silu_of_half(v * scale + shift)
                y = jnp.where(self.inside(row + iota(y.shape, 0) // wid), y, 0.0)
            for lane, part in enumerate((shifted(y, wid, 1), y, shifted(y, wid, -1))):
                lanes = slice(lane * ch, (lane + 1) * ch)
                self.put(buf, j, together, lanes, part.astype(buf.dtype))

    def keep_last(self, buf, before):
        wid, blk = self.wid, self.blk
        if self.pair:
            buf[:, :wid, :] = before[:, blk // 2 * wid:, :]
        else:
            buf[:2 * wid, :] = before[blk * wid:, :]

    def put(self, buf, j, together, lanes, part):
        wid = self.wid
        if self.pair:
            buf[j % 2, j // 2 * wid:(j // 2 + 1) * wid, lanes] = part
        else:
            buf[j * wid:(j + together) * wid, lanes] = part

    def buffer(self):
        n_px, ch = (self.blk + 2) * self.wid, self.ch
        shape = (2, n_px // 2, 3 * ch) if self.pair else (n_px, 3 * ch)
        return pltpu.VMEM(shape, F32 if self.wid < 16 else BF16)

    def product(self, buf, w_ref):
        m = self.blk * self.wid // (2 if self.pair else 1)
        if self.pair:
            lhs = jnp.concatenate([buf[t % 2, t // 2 * self.wid:t // 2 * self.wid + m, :] for t in range(4)], axis=1)
            return dot(lhs, w_ref[...])
        acc = None
        for t in range(3):
            part = dot(buf[t * self.wid:t * self.wid + m, :].astype(BF16), w_ref[t])
            acc = part if acc is None else acc + part
        return acc

    def run(self, bufs, work):
        n_blk = -(-self.n_out // self.blk)
        self.fill(bufs[0], 0)
        if n_blk > 1:
            def step(i, carry):
                self.fill(bufs[1], 2 * i + 1, bufs[0])
                work(bufs[0], 2 * i)
                self.fill(bufs[0], 2 * i + 2, bufs[1])
                work(bufs[1], 2 * i + 1)
                return carry
            repeat(n_blk // 2, step)
        if n_blk % 2:
            work(bufs[0], n_blk - 1)


def paired_weights(w_ref, wp_ref):
    oc = w_ref.shape[2]
    clear(wp_ref)
    k = w_ref.shape[1]
    for t in range(3):
        wp_ref[t * k:(t + 1) * k, :oc] = w_ref[t]
        wp_ref[(t + 1) * k:(t + 2) * k, oc:] = w_ref[t]


def conv_kernel(cfg, net, *refs):
    wid, h, blk, out_ext, pair, shortcut, stats, edge, skip_blk = cfg
    refs = iter(refs)
    x_ref, norm_tot_ref, norm_ref, w_ref = [next(refs) for _ in 'abcd']
    short_ref = next(refs) if shortcut else None
    skip_ref = next(refs) if skip_blk else None
    out_ref = next(refs)
    tot_ref = next(refs) if stats else None
    skip_out_ref = next(refs) if skip_blk else None
    buf0, buf1, s1_ref, s2_ref = [next(refs) for _ in 'abcd']
    wp_ref = next(refs) if pair else w_ref
    net_refs = list(refs)
    ch, oc = x_ref.shape[-1], w_ref.shape[2]
    n_out = h + 2 * out_ext
    coefs = norm_coefs(norm_tot_ref[...], norm_ref, ch, float(net.n * h * wid * (ch // GROUPS)))
    rows = Rows(net, x_ref, coefs, wid, h, 1 + out_ext, n_out, blk, pair)
    clear(s1_ref, s2_ref)
    if pair:
        paired_weights(w_ref, wp_ref)
    exact = n_out % blk == 0 and not out_ext

    def count(y, first_row, step):
        yf = y.astype(F32)
        if exact:
            s1_ref[...] += fold8(yf)
            s2_ref[...] += fold8(yf * yf)
            return
        for i, part in enumerate(jnp.split(yf, yf.shape[0] // wid)):
            r = first_row + step * i
            own = (r >= out_ext) & (r < h + out_ext)
            s1_ref[...] += jnp.where(own, fold8(part), 0.0)
            s2_ref[...] += jnp.where(own, fold8(part * part), 0.0)

    def work(buf, b):
        k0 = b * blk
        acc = rows.product(buf, wp_ref)
        if pair:
            for a in range(2):
                val = acc[:, a * oc:(a + 1) * oc]
                here = pl.ds(edge // 2 + k0 // 2, blk // 2)
                if shortcut:
                    val = short_ref[pl.ds(k0 // 2, blk // 2), a].reshape(val.shape) + val
                y = val.astype(BF16)
                out_ref[here, a] = y.reshape(blk // 2, wid, oc)
                if stats:
                    count(y, k0 + a, 2)
        else:
            if shortcut:
                acc = short_ref[aligned(k0 * wid, blk * wid, SUB), :].astype(F32) + acc
            y = acc.astype(BF16)
            out_ref[aligned((k0 + edge) * wid, blk * wid, SUB), :] = y
            if stats:
                count(y, k0, 1)
    rows.run((buf0, buf1), work)
    if out_ext:
        for at, at_edge in ((0, net.strip == 0), (n_out - 1, net.strip == net.n - 1)):
            where = out_ref.at[at // 2, at % 2] if pair else out_ref.at[pl.ds(at * wid, wid)]

            @pl.when(at_edge)
            def _():
                where[...] = jnp.zeros(where.shape, BF16)
    if stats:
        sides = None
        if edge:
            def part(row):
                return out_ref.at[row // 2] if pair else out_ref.at[pl.ds(row * wid, edge * wid)]
            sides = (part(edge), part(h), part(0), part(h + edge), *net_refs[3:])

        def skip_step(b, carry):
            here = aligned(b * skip_blk * wid, skip_blk * wid, SUB)
            skip_out_ref[here, :] = dot(x_ref[here, :], skip_ref[...])
            return carry

        def skip_all():
            repeat(skip_out_ref.shape[0] // (skip_blk * wid), skip_step)
        exchange(net, group_sums(s1_ref[...], s2_ref[...]), *net_refs[:3], tot_ref, sides, skip_all if skip_blk else None)


def conv(x, tot, norm, w, h, wid, n, blk, out_ext, stats, edge, pair, short, skip):
    ch, oc = w.shape[2:]
    args = [x, tot, norm, w.reshape(3, 3 * ch, oc)]
    for src in short:
        args.append(src.reshape(-1, 2, wid, src.shape[-1]) if pair else src)
    args += skip[:1]
    n_out = h + 2 * out_ext
    rows = -(-n_out // blk) * blk + 2 * edge
    outs = [jax.ShapeDtypeStruct((rows // 2, 2, wid, oc) if pair else (rows * wid, oc), BF16)]
    if stats:
        outs.append(TOTALS)
    cfg = (wid, h, blk, out_ext, pair, bool(short), stats, edge, skip[1] if skip else 0)
    if skip:
        outs.append(jax.ShapeDtypeStruct((skip[2] * wid, skip[0].shape[1]), F32))
    layout = Rows(None, x, None, wid, h, None, n_out, blk, pair)
    scratch = [layout.buffer(), layout.buffer(), *sum_scratch(oc)]
    if pair:
        scratch.append(pltpu.VMEM((12 * ch, 2 * oc), BF16))
    if stats:
        scratch += net_scratch(n, ((2, wid, oc) if pair else (edge * wid, oc)) if edge else None)
    return functools.partial(conv_kernel, cfg), args, outs, scratch


def upconv_kernel(cfg, net, x_ref, w_ref, out_ref, tot_ref, s1_ref, s2_ref, mix_ref, stat_ref, recv, sems):
    half, hs, blk = cfg
    oc = w_ref.shape[2]
    n_k = hs + 1
    mixed = half < BASE
    m, more = blk * half, (blk + 1) * half
    clear(s1_ref, s2_ref)

    def step(b, carry):
        k0 = jnp.minimum(b * blk, n_k - blk) if n_k > blk else 0
        x = x_ref[aligned(k0 * half, more, SUB), :]
        rows = []
        for dx in range(3):
            above, mid, below = [dot(x, w_ref[3 * dy + dx]) for dy in range(3)]
            both = above[:m] + below[half:]
            rows.append((both + mid[:m], both + mid[half:]))
        for a in range(2):
            left, at, right = [r[a] for r in rows]
            even = at + right + shifted(left, half, 1)
            odd = left + at + shifted(right, half, -1)
            for q, val in ((0, even), (1, odd)):
                y = val.astype(BF16)
                if mixed:
                    for c in range(0, oc, LANES):
                        mix_ref[a, c // LANES, pl.ds(q, m, stride=2), :] = val[:, c:c + LANES]
                else:
                    out_ref[pl.ds(k0, blk), a, q * half:(q + 1) * half, :] = y.reshape(blk, half, oc)
                yf = y.astype(F32)
                for i, part in enumerate(jnp.split(yf, blk)):
                    k = k0 + i
                    own = (k >= b * blk) & ((k < hs) if a else (k > 0))
                    s1_ref[...] += jnp.where(own, fold8(part), 0.0)
                    s2_ref[...] += jnp.where(own, fold8(part * part), 0.0)
            for c in range(0, oc if mixed else 0, LANES):
                out_ref[pl.ds(k0, blk), a, :, c:c + LANES] = mix_ref[a, c // LANES].astype(BF16).reshape(blk, 2 * half, LANES)
        return carry
    if n_k == blk:
        step(0, 0)
    else:
        repeat(-(-n_k // blk), step)
    exchange(net, group_sums(s1_ref[...], s2_ref[...]), stat_ref, recv, sems, tot_ref)


def upconv(x, w, hs, half, n, blk):
    ch, oc = w.shape[2:]
    n_k = hs + SUB
    outs = [jax.ShapeDtypeStruct((n_k, 2, 2 * half, oc), BF16), TOTALS]
    scratch = [*sum_scratch(oc), pltpu.VMEM((2, oc // LANES, 2 * blk * half if half < BASE else SUB, LANES), F32)]
    return functools.partial(upconv_kernel, (half, hs, blk)), [x, w.reshape(-1, ch, oc)], outs, scratch + net_scratch(n)


class Made:
    def __init__(self, part, index):
        self.part, self.index = part, index
        self.shape = part[2][index].shape


def launch(parts, net_shape, cid, mib, name):
    arrays = []
    for _, args, _, _ in parts:
        arrays += [a for a in args if not isinstance(a, Made) and not any(a is b for b in arrays)]
    outs = parts[-1][2]
    inner = [o for part in parts[:-1] for o in part[2]]

    def kernel(*refs):
        refs = iter(refs)
        given = [next(refs) for _ in arrays]
        last = [next(refs) for _ in outs]
        made = [[next(refs) for _ in part[2]] for part in parts[:-1]] + [last]
        net = Net(*net_shape)
        net.greet()

        def ref_of(arg):
            if isinstance(arg, Made):
                return [refs_[arg.index] for part, refs_ in zip(parts, made) if part is arg.part].pop()
            return [ref for a, ref in zip(arrays, given) if a is arg].pop()
        for part, own in zip(parts, made):
            run, args, _, scratch = part
            run(net, *[ref_of(a) for a in args], *own, *[next(refs) for _ in scratch])
        net.all_here()
    return pl.pallas_call(
        kernel, out_shape=outs, in_specs=[VMEM_SPEC] * len(arrays), out_specs=[VMEM_SPEC] * len(outs),
        scratch_shapes=[pltpu.VMEM(o.shape, o.dtype) for o in inner] + [x for part in parts for x in part[3]],
        compiler_params=comm_params(cid, mib), name=name,
    )(*arrays)


class QuarterRows(Rows):
    def keep_last(self, buf, before):
        buf[:, :2 * self.tile] = before[:, self.blk * self.tile:]

    def put(self, buf, j, together, lanes, part):
        n_q = buf.shape[0]
        here = self.tile // (self.wid // BASE)
        whole = part.reshape(self.wid // BASE, BASE, part.shape[1])
        for q in range(n_q):
            buf[q, j * self.tile:(j + 1) * self.tile, lanes] = whole[:, q * here:(q + 1) * here].reshape(self.tile, part.shape[1])


def last_kernel(cfg, x_ref, tot_ref, norm_ref, w_ref, out_ref, buf0, buf1, mine, recv, send_sems, recv_sems):
    net_shape, wid, h, blk, oc = cfg
    net = Net(*net_shape)
    barrier = pltpu.get_barrier_semaphore()
    cols = [lax.rem(net.col + k, net.n_col) for k in range(net.n_col)]
    for col in cols[1:]:
        pl.semaphore_signal(barrier, inc=1, device_id={'col': col}, device_id_type=MESH)
    ch = x_ref.shape[1]
    coefs = norm_coefs(tot_ref[...], norm_ref, ch, float(net.n * h * wid * (ch // GROUPS)))
    rows = QuarterRows(net, x_ref, coefs, wid, h, 1, h, blk, False)
    rows.tile = tile = wid // net.n_col
    m = blk * tile
    per = h * tile // LANES

    def work(buf, b):
        for q in range(net.n_col):
            z = dot_t(w_ref[...], buf[q])
            z = z[:SUB, :m] + z[SUB:16, tile:tile + m] + z[16:, 2 * tile:2 * tile + m]
            for c in range(oc):
                for t in range(m // LANES):
                    mine[q, pl.ds(c * per + b * (m // LANES) + t, 1), :] = z[c:c + 1, t * LANES:(t + 1) * LANES]
    rows.run((buf0, buf1), work)
    pl.semaphore_wait(barrier, net.n_col - 1)
    copies = []
    for k, col in enumerate(cols[1:]):
        copies.append(pltpu.make_async_remote_copy(
            src_ref=mine.at[col], dst_ref=recv.at[net.col], send_sem=send_sems.at[k], recv_sem=recv_sems.at[k],
            device_id={'col': col}, device_id_type=MESH))
        copies[-1].start()
    recv[net.col] = mine[net.col]
    for copy in copies:
        copy.wait()
    i, j = iota((LANES, LANES), 0), iota((LANES, LANES), 1)
    splits = wid // BASE
    lane, run = lax.rem(j, tile), j // tile
    src = run * tile + lax.rem(lane, 2) * (tile // 2) + lax.rem(lane // 2, splits // 2) * (tile // splits) + lane // splits
    perm = (i == src).astype(F32)
    for q in range(net.n_col):
        out_ref[q] = exact_dot(recv[q], perm)


def last_conv(x, tot, norm, w, h, wid, net_shape, blk, cid):
    n_col = net_shape[1]
    ch, oc = w.shape[2:]
    wt = jnp.zeros((3, SUB, 3 * ch), BF16).at[:, :oc].set(w.reshape(3, 3 * ch, oc).transpose(0, 2, 1))
    buf = pltpu.VMEM((n_col, (blk + 2) * wid // n_col, 3 * ch), BF16)
    shape = (n_col, oc * h * wid // n_col // LANES, LANES)
    return pl.pallas_call(
        functools.partial(last_kernel, (net_shape, wid, h, blk, oc)),
        out_shape=jax.ShapeDtypeStruct(shape, F32),
        in_specs=[VMEM_SPEC] * 4, out_specs=VMEM_SPEC,
        scratch_shapes=[buf, buf, pltpu.VMEM(shape, F32), pltpu.VMEM(shape, F32)] + [pltpu.SemaphoreType.DMA((n_col,))] * 2,
        compiler_params=comm_params(cid, 28),
        name='last_conv',
    )(x, tot, norm, wt.reshape(-1, 3 * ch))


def device_body(net_shape, tokens, mod_vec, w_fc1, w_fc2, w_final, conv_in, norm_attn, w_qkv, w_proj,
                norm0_a, conv0_a, norm0_b, conv0_b, upconv_0, norm1_a, conv1_a, norm1_b, conv1_b, upconv_1,
                norm2_a, conv2_a, norm2_b, conv2_b, skip_2, upconv_2, norm3_a, conv3_a, norm3_b, conv3_b,
                skip_3, norm_out, conv_out):
    n_col = net_shape[1]
    trows, tok_w, d = tokens.shape
    full = mlp(tokens.reshape(-1, d), tok_w, mod_vec, w_fc1, w_fc2, w_final, net_shape, 1)
    h, wid = 2 * trows, 2 * tok_w
    f, tot = attention(full.reshape(-1, full.shape[-1]), conv_in, norm_attn, w_qkv, w_proj, net_shape, 2)
    u = f.reshape(-1, f.shape[-1])
    blocks = [(norm0_a, conv0_a, norm0_b, conv0_b, (), upconv_0, h, h + 2, h + 1, 15),
              (norm1_a, conv1_a, norm1_b, conv1_b, (), upconv_1, 16, 11, 13, 13),
              (norm2_a, conv2_a, norm2_b, conv2_b, (skip_2,), upconv_2, 16, 10, 10, 20),
              (norm3_a, conv3_a, norm3_b, conv3_b, (skip_3,), None, 16, 16, 0, 24)]
    cid, n = 3, net_shape[0] * n_col
    for norm_a, conv_a, norm_b, conv_b, skip, up, blk_a, blk_b, blk_up, mib in blocks:
        last = up is None
        rows = -(-(h + 2) // blk_b) * blk_b
        skip = [(m, rows // (SUB if rows % SUB == 0 else 5), rows) for m in skip]
        first = conv(u, tot, norm_a, conv_a, h, wid, n, blk_a, 0, True, 2, last, (), *skip or [()])
        name = 'level_w%d' % wid
        if last:
            g, tot, *short = launch([first], net_shape, cid, mib, name + 'a')
            g, short = g.reshape(-1, g.shape[-1]), short
        else:
            g, tot, *short = [Made(first, i) for i, _ in enumerate(first[2])]
        second = conv(g, tot, norm_b, conv_b, h, wid, n, blk_b, 1, last, 0, last, short or (u,), ())
        if last:
            f, tot = launch([second], net_shape, cid + 1, mib, name + 'b')
        else:
            third = upconv(Made(second, 0), up, h, wid, n, blk_up)
            u, tot = launch([first, second, third], net_shape, cid, mib, name)
            u = u.reshape(-1, u.shape[-1])
            h, wid = 2 * h, 2 * wid
        cid += 2
    tile = last_conv(f.reshape(-1, f.shape[-1]), tot, norm_out, conv_out, h, wid, net_shape, 16, cid)
    tile = tile.reshape(n_col, -1, h, wid // n_col).transpose(0, 2, 3, 1)
    return tile.reshape(n_col * h, wid // n_col, -1)


def solution(mesh):
    body_fn = functools.partial(device_body, (mesh.shape['row'], mesh.shape['col']))
    tok_spec = P(('batch', 'row', 'col'), None, None)
    out_spec = P(('batch', 'row'), 'col', None)
    return jax.shard_map(body_fn, mesh=mesh, in_specs=(tok_spec,) + (P(),) * 31, out_specs=out_spec, check_vma=False)
```

```python
import functools
import jax
import jax.numpy as jnp
from jax import lax
from jax.experimental import pallas as pl
from jax.experimental.pallas import tpu as pltpu
from jax.sharding import PartitionSpec as P

GROUPS = 32
LOG2_E = 1.4426950408889634
LANES = 128
SUB = 8
BASE = 16
F32, BF16 = jnp.float32, jnp.bfloat16
MESH = pl.DeviceIdType.MESH
VMEM_SPEC = pl.BlockSpec(memory_space=pltpu.VMEM)
MIB = 1 << 20
TOTALS = jax.ShapeDtypeStruct((1, LANES), F32)


def dot(a, b):
    return jnp.dot(a, b, preferred_element_type=F32)


def dot_t(a, b):
    return lax.dot_general(a, b, (((1,), (1,)), ((), ())), preferred_element_type=F32)


def exact_dot(a, b):
    return jnp.dot(a, b, preferred_element_type=F32, precision=lax.Precision.HIGHEST)


def clear(*refs):
    for ref in refs:
        ref[...] = jnp.zeros_like(ref)


def repeat(count, step):
    lax.fori_loop(0, count, step, 0)


def iota(shape, dim):
    return lax.broadcasted_iota(jnp.int32, shape, dim)


def aligned(first, size, unit):
    return pl.ds(pl.multiple_of(first, unit), size)


def layer_norm(v):
    mean = jnp.mean(v, axis=-1, keepdims=True)
    var = jnp.mean(jnp.square(v - mean), axis=-1, keepdims=True)
    return (v - mean) * lax.rsqrt(var + 1e-6)


def silu_of_half(half):
    return half + half * jnp.tanh(half)


class Net:
    def __init__(self, n_row, n_col):
        self.n_row, self.n_col = n_row, n_col
        self.n = n_row * n_col
        self.row, self.col = lax.axis_index('row'), lax.axis_index('col')
        self.strip = self.row * n_col + self.col
        self.met = False

    def for_others(self, act, row_step=1):
        cols = [lax.rem(self.col + k, self.n_col) for k in range(self.n_col)]
        n_row = self.n_row // row_step

        def step(k, carry):
            row = lax.rem(self.row + (1 + lax.rem(k + n_row // 2 - 1, n_row - 1)) * row_step, self.n_row)
            for col in cols:
                act({'row': row, 'col': col})
            return carry
        repeat(n_row - 1, step)
        for col in cols[1:]:
            act({'row': self.row, 'col': col})
        return self.n // row_step - 1

    def beside(self, ahead):
        other = lax.rem(self.strip + ahead, self.n)
        return {'row': other // self.n_col, 'col': lax.rem(other, self.n_col)}

    def greet(self):
        barrier = pltpu.get_barrier_semaphore()
        self.for_others(lambda device: pl.semaphore_signal(barrier, inc=1, device_id=device, device_id_type=MESH))

    def all_here(self):
        if not self.met:
            pl.semaphore_wait(pltpu.get_barrier_semaphore(), self.n - 1)
        self.met = True

    def to_others(self, src, recv, sems, row_step=1):
        count = self.for_others(lambda device: send(src, recv.at[self.strip], sems, device).start(), row_step)

        def wait():
            done = recv.at[pl.ds(0, count)]
            for side in range(2):
                pltpu.make_async_copy(done, done, sems.at[side]).wait()
        return wait


def send(src, dst, sems, device):
    return pltpu.make_async_remote_copy(
        src_ref=src, dst_ref=dst, send_sem=sems.at[0], recv_sem=sems.at[1], device_id=device, device_id_type=MESH)


PAIR_SEM = pltpu.SemaphoreType.DMA((2,))


def net_scratch(n, edge_shape=None):
    scratch = [pltpu.VMEM((1, LANES), F32), pltpu.VMEM((n, 1, LANES), F32), PAIR_SEM]
    if edge_shape is not None:
        scratch += [pltpu.VMEM((2,) + edge_shape, BF16), PAIR_SEM, PAIR_SEM]
    return scratch


def exchange(net, stat, stat_ref, recv, sems, tot_ref, sides=None, meanwhile=None):
    stat_ref[...] = stat
    net.all_here()
    wait = net.to_others(stat_ref, recv, sems)
    side_copies = []
    if sides is not None:
        first, last, top, bottom, hrecv, down_sems, up_sems = sides
        side_copies = [(send(src, hrecv.at[side], pair, net.beside(ahead)), dst, side) for side, (src, dst, pair, ahead)
                       in enumerate(((last, top, down_sems, 1), (first, bottom, up_sems, net.n - 1)))]
    for copy, _, _ in side_copies:
        copy.start()
    recv[net.strip] = stat
    if meanwhile:
        meanwhile()
    wait()
    tot_ref[...] = jnp.sum(recv[...], axis=0)
    for copy, dst, side in side_copies:
        copy.wait()
        dst[...] = hrecv[side]


def sum_scratch(ch):
    return [pltpu.VMEM((SUB, ch), F32)] * 2


def comm_params(cid, mib):
    return pltpu.CompilerParams(collective_id=cid, has_side_effects=True, vmem_limit_bytes=mib * MIB)


def mlp_kernel(net_shape, x_ref, mod_ref, w1_ref, w2_ref, wf_ref, o_ref,
               w1_buf, w2_buf, act_ref, acc_ref, part_ref, tok_ref, mix_ref, recv, w_sems, sems, swap_sems, pass_sems):
    net = Net(*net_shape)
    n_buf, blk = w1_buf.shape[0], w1_buf.shape[2]
    n_cut = w1_ref.shape[1] // blk // 2
    core = lax.rem(net.row, 2)
    partner = {'row': net.row + 1 - 2 * core, 'col': net.col}
    n_tok = x_ref.shape[0]

    def loads(i):
        part, slot = aligned((core * n_cut + i) * blk, blk, blk), lax.rem(i, n_buf)
        return [pltpu.make_async_copy(w1_ref.at[:, part], w1_buf.at[slot], w_sems.at[0, slot]),
                pltpu.make_async_copy(w2_ref.at[part], w2_buf.at[slot], w_sems.at[1, slot])]
    for i in range(n_cut):
        for load in loads(i):
            load.start()
    net.greet()
    shift1, scale1, gate1, shift2, scale2 = [mod_ref[pl.ds(i, 1)] for i in range(5)]
    x = x_ref[...].astype(F32)
    act = (layer_norm(x) * (1.0 + scale1) + shift1).astype(BF16)
    act_ref[0] = act
    clear(acc_ref)
    net.all_here()
    swap = send(act_ref.at[0], act_ref.at[1], swap_sems.at[0], partner)
    swap.start()
    swap.wait()

    def step(i, carry):
        load1, load2 = loads(i)
        slot = lax.rem(i, n_buf)
        load1.wait()
        hid = jax.nn.gelu(dot(act_ref[...].reshape(2 * n_tok, -1), w1_buf[slot]), approximate=True).astype(BF16)
        load2.wait()
        acc_ref[...] += dot(hid, w2_buf[slot]).reshape(acc_ref.shape)
        return carry
    repeat(n_cut, step)
    swap = send(acc_ref.at[1], part_ref, swap_sems.at[1], partner)
    swap.start()
    swap.wait()
    acc = acc_ref[0] + part_ref[...]
    y = (x + gate1 * acc).astype(BF16)
    fin = (layer_norm(y.astype(F32)) * (1.0 + scale2) + shift2).astype(BF16)
    tok_ref[...] = dot_t(fin, wf_ref[...])
    rows, part = mix_ref.shape[0] // 2, wf_ref.shape[0] // 2
    tok_w = tok_ref.shape[0] // rows
    toks = [tok_ref[pl.ds(j, rows, stride=tok_w), :] for j in range(tok_w)]
    for p in range(2):
        mix_ref[pl.ds(p, rows, stride=2), :] = jnp.concatenate([t[:, p * part:(p + 1) * part] for t in toks], axis=1)
    recv[net.strip] = mix_ref[...].astype(BF16)
    net.to_others(recv.at[net.strip], recv, sems, 2)()
    copies = []
    for i in range(net.n_row // 2):
        line = recv.at[pl.ds((2 * i + core) * net.n_col, net.n_col)]
        copies.append(send(line, line, pass_sems.at[i], partner))
        copies[-1].start()
    for copy in copies:
        copy.wait()
    o_ref[...] = recv[...]


def mlp(x, tok_w, mod_vec, w_fc1, w_fc2, w_final, net_shape, cid):
    n = net_shape[0] * net_shape[1]
    n_tok, d = x.shape
    hid, patch = w_fc1.shape[1], w_final.shape[1]
    n_buf = 4
    blk = hid // (2 * n_buf)
    rows = 2 * n_tok // tok_w
    lat = (rows, n_tok * patch // rows)
    hbm = pl.BlockSpec(memory_space=pltpu.HBM)
    return pl.pallas_call(
        functools.partial(mlp_kernel, net_shape),
        out_shape=jax.ShapeDtypeStruct((n,) + lat, BF16),
        in_specs=[VMEM_SPEC, VMEM_SPEC, hbm, hbm, VMEM_SPEC],
        out_specs=VMEM_SPEC,
        scratch_shapes=[pltpu.VMEM((n_buf, d, blk), BF16), pltpu.VMEM((n_buf, blk, d), BF16),
                        pltpu.VMEM((2,) + x.shape, BF16), pltpu.VMEM((2,) + x.shape, F32), pltpu.VMEM(x.shape, F32),
                        pltpu.VMEM((n_tok, patch), F32), pltpu.VMEM(lat, F32), pltpu.VMEM((n,) + lat, BF16),
                        pltpu.SemaphoreType.DMA((2, n_buf)), PAIR_SEM, pltpu.SemaphoreType.DMA((2, 2)), pltpu.SemaphoreType.DMA((net_shape[0] // 2, 2))],
        compiler_params=comm_params(cid, 46),
        name='mlp',
    )(x, mod_vec, w_fc1, w_fc2, w_final.T)


def in_group(channel, lane, per):
    return ((channel >= lane * per) & (channel < lane * per + per)).astype(F32)


def group_sums(s1, s2):
    ch = s1.shape[1]
    shape = (ch, LANES)
    both = [exact_dot(s, in_group(iota(shape, 0), iota(shape, 1) - at, ch // GROUPS))
            for s, at in ((s1, 0), (s2, GROUPS))]
    return jnp.sum(both[0] + both[1], axis=0, keepdims=True)


def norm_coefs(tot, norm_ref, ch, count):
    avg = jnp.broadcast_to(tot / count, (SUB, LANES))
    shape = (LANES, ch)
    mean, square = [exact_dot(avg, in_group(iota(shape, 1), iota(shape, 0) - at, ch // GROUPS)) for at in (0, GROUPS)]
    scale = lax.rsqrt(square - jnp.square(mean) + 1e-6) * norm_ref[0:1]
    return mean[0:1], scale[0:1], norm_ref[1:2]


def fold8(v):
    return jnp.sum(v.reshape(v.shape[0] // SUB, SUB, v.shape[1]), axis=0)


def attention_kernel(net_shape, lat_ref, win_ref, norm_ref, wqkv_ref, wproj_ref, out_ref, tot_ref,
                     cols_ref, toe_ref, fmap_ref, loc_ref, sc_ref, s1_ref, s2_ref, m_ref, l_ref, acc_ref,
                     stat_ref, recv, sems, *halo_refs):
    net = Net(*net_shape)
    net.greet()
    rows = lat_ref.shape[0]
    lat_c, ch = win_ref.shape[1:]
    wid = lat_ref.shape[1] // lat_c
    own = rows // net.n
    lat = lat_ref[...].astype(F32)
    idx = iota(lat.shape, 0)
    cols_ref[...] = jnp.concatenate([jnp.where(idx == 0, 0.0, pltpu.roll(lat, 1, 0)), lat,
                                     jnp.where(idx == rows - 1, 0.0, pltpu.roll(lat, rows - 1, 0))], axis=1).astype(BF16)
    clear(toe_ref)
    for x in range(wid):
        for tap in range(9):
            src = x + tap % 3 - 1
            if 0 <= src < wid:
                toe_ref[x, pl.ds(tap // 3 * LANES + src * lat_c, lat_c), :] = win_ref[tap]
    clear(s1_ref, s2_ref)
    blk = 1024
    per_col = rows // blk

    def conv_step(i, carry):
        y = dot(cols_ref[aligned(lax.rem(i, per_col) * blk, blk, blk), :], toe_ref[i // per_col]).astype(BF16)
        fmap_ref[aligned(i * blk, blk, blk), :] = y
        yf = y.astype(F32)
        s1_ref[...] += fold8(yf)
        s2_ref[...] += fold8(yf * yf)
        return carry
    repeat(wid * per_col, conv_step)
    mean, scale, shift = norm_coefs(group_sums(s1_ref[...], s2_ref[...]), norm_ref, ch, float(rows * wid * (ch // GROUPS)))

    for x in range(wid):
        loc_ref[x * own:(x + 1) * own, :] = fmap_ref[aligned(x * rows + net.strip * own, own, own), :]
    nl = ((loc_ref[...].astype(F32) - mean) * scale + shift).astype(BF16)
    q = dot(nl, wqkv_ref[:, :ch]).astype(BF16)
    qk = (dot_t(q, wqkv_ref[:, ch:2 * ch]) * (scale * (float(ch) ** -0.5 * LOG2_E))).astype(BF16)
    nk, n_q, kb = sc_ref.shape
    m_ref[...] = jnp.full_like(m_ref, -jnp.inf)

    def score_step(i, carry):
        s = dot_t(qk, fmap_ref[aligned(i * kb, kb, kb), :])
        sc_ref[i] = s
        m = m_ref[...]
        for j in range(kb // LANES):
            m = jnp.maximum(m, s[:, j * LANES:(j + 1) * LANES])
        m_ref[...] = m
        return carry
    repeat(nk, score_step)
    m_ref[...] = jnp.broadcast_to(jnp.max(m_ref[...], axis=1, keepdims=True), m_ref.shape)
    clear(l_ref, acc_ref)

    def value_step(i, carry):
        m = m_ref[...]
        tot_l = l_ref[...]
        parts = []
        for j in range(kb // LANES):
            e = jnp.exp2(sc_ref[i, :, j * LANES:(j + 1) * LANES] - m).astype(BF16)
            tot_l = tot_l + e.astype(F32)
            parts.append(e)
        l_ref[...] = tot_l
        acc_ref[...] += dot(jnp.concatenate(parts, axis=1), fmap_ref[aligned(i * kb, kb, kb), :])
        return carry
    repeat(nk, value_step)
    pn = acc_ref[...] / jnp.sum(l_ref[...], axis=1, keepdims=True)
    pn = ((pn - mean) * scale + shift).astype(BF16)
    att = dot(pn, wqkv_ref[:, 2 * ch:]).astype(BF16)
    out = (loc_ref[...].astype(F32) + dot(att, wproj_ref[...])).astype(BF16)
    i, j = iota((n_q, n_q), 0), iota((n_q, n_q), 1)
    perm = (j == lax.rem(i, wid) * own + i // wid).astype(BF16)
    of = dot(perm, out)
    out_ref[pl.ds(1, own)] = of.astype(BF16).reshape(own, wid, ch)
    exchange(net, group_sums(fold8(of), fold8(of * of)), stat_ref, recv, sems, tot_ref,
             (out_ref.at[1], out_ref.at[own], out_ref.at[0], out_ref.at[own + 1], *halo_refs))


def attention(lat, conv_in, norm, w_qkv, w_proj, net_shape, cid):
    n = net_shape[0] * net_shape[1]
    rows = lat.shape[0]
    lat_c, ch = conv_in.shape[2:]
    wid = lat.shape[1] // lat_c
    own = rows // n
    n_q = own * wid
    kb = 2048
    return pl.pallas_call(
        functools.partial(attention_kernel, net_shape),
        out_shape=[jax.ShapeDtypeStruct((own + 2, wid, ch), BF16), TOTALS],
        in_specs=[VMEM_SPEC] * 5, out_specs=[VMEM_SPEC] * 2,
        scratch_shapes=[pltpu.VMEM((rows, 3 * LANES), BF16), pltpu.VMEM((wid, 3 * LANES, ch), BF16),
                        pltpu.VMEM((rows * wid, ch), BF16), pltpu.VMEM((n_q, ch), BF16),
                        pltpu.VMEM((rows * wid // kb, n_q, kb), F32),
                        *sum_scratch(ch),
                        pltpu.VMEM((n_q, LANES), F32), pltpu.VMEM((n_q, LANES), F32), pltpu.VMEM((n_q, ch), F32)]
        + net_scratch(n, (wid, ch)),
        compiler_params=comm_params(cid, 27),
        name='attention',
    )(lat, conv_in.reshape(9, lat_c, ch), norm, w_qkv, w_proj)


def shifted(y, wid, by):
    n_px, ch = y.shape
    if wid > BASE:
        even, odd = jnp.split(y.reshape(n_px // wid, 2, wid // 2, ch), 2, axis=1)
        far = shifted((odd if by == 1 else even).reshape(n_px // 2, ch), wid // 2, by).reshape(even.shape)
        return jnp.concatenate([far, even] if by == 1 else [odd, far], axis=1).reshape(n_px, ch)
    tiles = pltpu.roll(y, by % n_px, 0).reshape(n_px // wid, wid // SUB, SUB, ch)
    at, sub = (0, 0) if by > 0 else (wid // SUB - 1, 7)
    edge = tiles[:, at:at + 1]
    edge = jnp.where(iota(edge.shape, 2) == sub, 0.0, edge)
    parts = [tiles[:, :at], edge, tiles[:, at + 1:]]
    return jnp.concatenate([p for p in parts if p.shape[1]], axis=1).reshape(n_px, ch)


class Rows:
    def __init__(self, net, x_ref, coefs, wid, h, pad, n_out, blk, pair):
        self.net, self.x_ref, self.coefs, self.wid, self.h, self.pad = net, x_ref, coefs, wid, h, pad
        self.n_out, self.blk, self.pair = n_out, blk, pair
        self.ch = x_ref.shape[-1]

    def inside(self, row):
        net = self.net
        return ((row >= self.pad) | (net.strip > 0)) & ((row < self.h + self.pad) | (net.strip < net.n - 1))

    def fill(self, buf, b, before=None):
        mean, scale, shift = self.coefs
        scale = 0.5 * scale
        shift = 0.5 * shift - mean * scale
        wid, ch, blk = self.wid, self.ch, self.blk
        if before is not None:
            self.keep_last(buf, before)
        together = -(-BASE // wid)
        for j in range(2 * (before is not None), blk + 2, together):
            row = b * blk + j
            if self.n_out > blk:
                row = jnp.minimum(row, self.n_out + 1)
            v = self.x_ref[aligned(row * wid, together * wid, SUB), :].astype(F32)
            if together == 1:
                keep = jnp.where(self.inside(row), 1.0, 0.0)
                y = silu_of_half(v * (scale * keep) + shift * keep)
            else:
                y = silu_of_half(v * scale + shift)
                y = jnp.where(self.inside(row + iota(y.shape, 0) // wid), y, 0.0)
            for lane, part in enumerate((shifted(y, wid, 1), y, shifted(y, wid, -1))):
                lanes = slice(lane * ch, (lane + 1) * ch)
                self.put(buf, j, together, lanes, part.astype(buf.dtype))

    def keep_last(self, buf, before):
        wid, blk = self.wid, self.blk
        if self.pair:
            buf[:, :wid, :] = before[:, blk // 2 * wid:, :]
        else:
            buf[:2 * wid, :] = before[blk * wid:, :]

    def put(self, buf, j, together, lanes, part):
        wid = self.wid
        if self.pair:
            buf[j % 2, j // 2 * wid:(j // 2 + 1) * wid, lanes] = part
        else:
            buf[j * wid:(j + together) * wid, lanes] = part

    def buffer(self):
        n_px, ch = (self.blk + 2) * self.wid, self.ch
        shape = (2, n_px // 2, 3 * ch) if self.pair else (n_px, 3 * ch)
        return pltpu.VMEM(shape, F32 if self.wid < 16 else BF16)

    def product(self, buf, w_ref):
        m = self.blk * self.wid // (2 if self.pair else 1)
        if self.pair:
            lhs = jnp.concatenate([buf[t % 2, t // 2 * self.wid:t // 2 * self.wid + m, :] for t in range(4)], axis=1)
            return dot(lhs, w_ref[...])
        acc = None
        for t in range(3):
            part = dot(buf[t * self.wid:t * self.wid + m, :].astype(BF16), w_ref[t])
            acc = part if acc is None else acc + part
        return acc

    def run(self, bufs, work):
        n_blk = -(-self.n_out // self.blk)
        self.fill(bufs[0], 0)
        if n_blk > 1:
            def step(i, carry):
                self.fill(bufs[1], 2 * i + 1, bufs[0])
                work(bufs[0], 2 * i)
                self.fill(bufs[0], 2 * i + 2, bufs[1])
                work(bufs[1], 2 * i + 1)
                return carry
            repeat(n_blk // 2, step)
        if n_blk % 2:
            work(bufs[0], n_blk - 1)


def paired_weights(w_ref, wp_ref):
    oc = w_ref.shape[2]
    clear(wp_ref)
    k = w_ref.shape[1]
    for t in range(3):
        wp_ref[t * k:(t + 1) * k, :oc] = w_ref[t]
        wp_ref[(t + 1) * k:(t + 2) * k, oc:] = w_ref[t]


def conv_kernel(cfg, net, *refs):
    wid, h, blk, out_ext, pair, shortcut, stats, edge, skip_blk = cfg
    refs = iter(refs)
    x_ref, norm_tot_ref, norm_ref, w_ref = [next(refs) for _ in 'abcd']
    short_ref = next(refs) if shortcut else None
    skip_ref = next(refs) if skip_blk else None
    out_ref = next(refs)
    tot_ref = next(refs) if stats else None
    skip_out_ref = next(refs) if skip_blk else None
    buf0, buf1, s1_ref, s2_ref = [next(refs) for _ in 'abcd']
    wp_ref = next(refs) if pair else w_ref
    net_refs = list(refs)
    ch, oc = x_ref.shape[-1], w_ref.shape[2]
    n_out = h + 2 * out_ext
    coefs = norm_coefs(norm_tot_ref[...], norm_ref, ch, float(net.n * h * wid * (ch // GROUPS)))
    rows = Rows(net, x_ref, coefs, wid, h, 1 + out_ext, n_out, blk, pair)
    clear(s1_ref, s2_ref)
    if pair:
        paired_weights(w_ref, wp_ref)
    exact = n_out % blk == 0 and not out_ext

    def count(y, first_row, step):
        yf = y.astype(F32)
        if exact:
            s1_ref[...] += fold8(yf)
            s2_ref[...] += fold8(yf * yf)
            return
        for i, part in enumerate(jnp.split(yf, yf.shape[0] // wid)):
            r = first_row + step * i
            own = (r >= out_ext) & (r < h + out_ext)
            s1_ref[...] += jnp.where(own, fold8(part), 0.0)
            s2_ref[...] += jnp.where(own, fold8(part * part), 0.0)

    def work(buf, b):
        k0 = b * blk
        acc = rows.product(buf, wp_ref)
        if pair:
            for a in range(2):
                val = acc[:, a * oc:(a + 1) * oc]
                here = pl.ds(edge // 2 + k0 // 2, blk // 2)
                if shortcut:
                    val = short_ref[pl.ds(k0 // 2, blk // 2), a].reshape(val.shape) + val
                y = val.astype(BF16)
                out_ref[here, a] = y.reshape(blk // 2, wid, oc)
                if stats:
                    count(y, k0 + a, 2)
        else:
            if shortcut:
                acc = short_ref[aligned(k0 * wid, blk * wid, SUB), :].astype(F32) + acc
            y = acc.astype(BF16)
            out_ref[aligned((k0 + edge) * wid, blk * wid, SUB), :] = y
            if stats:
                count(y, k0, 1)
    rows.run((buf0, buf1), work)
    if out_ext:
        for at, at_edge in ((0, net.strip == 0), (n_out - 1, net.strip == net.n - 1)):
            where = out_ref.at[at // 2, at % 2] if pair else out_ref.at[pl.ds(at * wid, wid)]

            @pl.when(at_edge)
            def _():
                where[...] = jnp.zeros(where.shape, BF16)
    if stats:
        sides = None
        if edge:
            def part(row):
                return out_ref.at[row // 2] if pair else out_ref.at[pl.ds(row * wid, edge * wid)]
            sides = (part(edge), part(h), part(0), part(h + edge), *net_refs[3:])

        def skip_step(b, carry):
            here = aligned(b * skip_blk * wid, skip_blk * wid, SUB)
            skip_out_ref[here, :] = dot(x_ref[here, :], skip_ref[...])
            return carry

        def skip_all():
            repeat(skip_out_ref.shape[0] // (skip_blk * wid), skip_step)
        exchange(net, group_sums(s1_ref[...], s2_ref[...]), *net_refs[:3], tot_ref, sides, skip_all if skip_blk else None)


def conv(x, tot, norm, w, h, wid, n, blk, out_ext, stats, edge, pair, short, skip):
    ch, oc = w.shape[2:]
    args = [x, tot, norm, w.reshape(3, 3 * ch, oc)]
    for src in short:
        args.append(src.reshape(-1, 2, wid, src.shape[-1]) if pair else src)
    args += skip[:1]
    n_out = h + 2 * out_ext
    rows = -(-n_out // blk) * blk + 2 * edge
    outs = [jax.ShapeDtypeStruct((rows // 2, 2, wid, oc) if pair else (rows * wid, oc), BF16)]
    if stats:
        outs.append(TOTALS)
    cfg = (wid, h, blk, out_ext, pair, bool(short), stats, edge, skip[1] if skip else 0)
    if skip:
        outs.append(jax.ShapeDtypeStruct((skip[2] * wid, skip[0].shape[1]), F32))
    layout = Rows(None, x, None, wid, h, None, n_out, blk, pair)
    scratch = [layout.buffer(), layout.buffer(), *sum_scratch(oc)]
    if pair:
        scratch.append(pltpu.VMEM((12 * ch, 2 * oc), BF16))
    if stats:
        scratch += net_scratch(n, ((2, wid, oc) if pair else (edge * wid, oc)) if edge else None)
    return functools.partial(conv_kernel, cfg), args, outs, scratch


def upconv_kernel(cfg, net, x_ref, w_ref, out_ref, tot_ref, s1_ref, s2_ref, mix_ref, stat_ref, recv, sems):
    half, hs, blk = cfg
    oc = w_ref.shape[2]
    n_k = hs + 1
    mixed = half < BASE
    m, more = blk * half, (blk + 1) * half
    clear(s1_ref, s2_ref)

    def step(b, carry):
        k0 = jnp.minimum(b * blk, n_k - blk) if n_k > blk else 0
        x = x_ref[aligned(k0 * half, more, SUB), :]
        rows = []
        for dx in range(3):
            above, mid, below = [dot(x, w_ref[3 * dy + dx]) for dy in range(3)]
            both = above[:m] + below[half:]
            rows.append((both + mid[:m], both + mid[half:]))
        for a in range(2):
            left, at, right = [r[a] for r in rows]
            even = at + right + shifted(left, half, 1)
            odd = left + at + shifted(right, half, -1)
            for q, val in ((0, even), (1, odd)):
                y = val.astype(BF16)
                if mixed:
                    for c in range(0, oc, LANES):
                        mix_ref[a, c // LANES, pl.ds(q, m, stride=2), :] = val[:, c:c + LANES]
                else:
                    out_ref[pl.ds(k0, blk), a, q * half:(q + 1) * half, :] = y.reshape(blk, half, oc)
                yf = y.astype(F32)
                for i, part in enumerate(jnp.split(yf, blk)):
                    k = k0 + i
                    own = (k >= b * blk) & ((k < hs) if a else (k > 0))
                    s1_ref[...] += jnp.where(own, fold8(part), 0.0)
                    s2_ref[...] += jnp.where(own, fold8(part * part), 0.0)
            for c in range(0, oc if mixed else 0, LANES):
                out_ref[pl.ds(k0, blk), a, :, c:c + LANES] = mix_ref[a, c // LANES].astype(BF16).reshape(blk, 2 * half, LANES)
        return carry
    if n_k == blk:
        step(0, 0)
    else:
        repeat(-(-n_k // blk), step)
    exchange(net, group_sums(s1_ref[...], s2_ref[...]), stat_ref, recv, sems, tot_ref)


def upconv(x, w, hs, half, n, blk):
    ch, oc = w.shape[2:]
    n_k = hs + SUB
    outs = [jax.ShapeDtypeStruct((n_k, 2, 2 * half, oc), BF16), TOTALS]
    scratch = [*sum_scratch(oc), pltpu.VMEM((2, oc // LANES, 2 * blk * half if half < BASE else SUB, LANES), F32)]
    return functools.partial(upconv_kernel, (half, hs, blk)), [x, w.reshape(-1, ch, oc)], outs, scratch + net_scratch(n)


class Made:
    def __init__(self, part, index):
        self.part, self.index = part, index
        self.shape = part[2][index].shape


def launch(parts, net_shape, cid, mib, name):
    arrays = []
    for _, args, _, _ in parts:
        arrays += [a for a in args if not isinstance(a, Made) and not any(a is b for b in arrays)]
    outs = parts[-1][2]
    inner = [o for part in parts[:-1] for o in part[2]]

    def kernel(*refs):
        refs = iter(refs)
        given = [next(refs) for _ in arrays]
        last = [next(refs) for _ in outs]
        made = [[next(refs) for _ in part[2]] for part in parts[:-1]] + [last]
        net = Net(*net_shape)
        net.greet()

        def ref_of(arg):
            if isinstance(arg, Made):
                return [refs_[arg.index] for part, refs_ in zip(parts, made) if part is arg.part].pop()
            return [ref for a, ref in zip(arrays, given) if a is arg].pop()
        for part, own in zip(parts, made):
            run, args, _, scratch = part
            run(net, *[ref_of(a) for a in args], *own, *[next(refs) for _ in scratch])
        net.all_here()
    return pl.pallas_call(
        kernel, out_shape=outs, in_specs=[VMEM_SPEC] * len(arrays), out_specs=[VMEM_SPEC] * len(outs),
        scratch_shapes=[pltpu.VMEM(o.shape, o.dtype) for o in inner] + [x for part in parts for x in part[3]],
        compiler_params=comm_params(cid, mib), name=name,
    )(*arrays)


class QuarterRows(Rows):
    def keep_last(self, buf, before):
        buf[:, :2 * self.tile] = before[:, self.blk * self.tile:]

    def put(self, buf, j, together, lanes, part):
        n_q = buf.shape[0]
        here = self.tile // (self.wid // BASE)
        whole = part.reshape(self.wid // BASE, BASE, part.shape[1])
        for q in range(n_q):
            buf[q, j * self.tile:(j + 1) * self.tile, lanes] = whole[:, q * here:(q + 1) * here].reshape(self.tile, part.shape[1])


def last_kernel(cfg, x_ref, tot_ref, norm_ref, w_ref, out_ref, buf0, buf1, mine, recv, send_sems, recv_sems):
    net_shape, wid, h, blk, oc = cfg
    net = Net(*net_shape)
    barrier = pltpu.get_barrier_semaphore()
    cols = [lax.rem(net.col + k, net.n_col) for k in range(net.n_col)]
    for col in cols[1:]:
        pl.semaphore_signal(barrier, inc=1, device_id={'col': col}, device_id_type=MESH)
    ch = x_ref.shape[1]
    coefs = norm_coefs(tot_ref[...], norm_ref, ch, float(net.n * h * wid * (ch // GROUPS)))
    rows = QuarterRows(net, x_ref, coefs, wid, h, 1, h, blk, False)
    rows.tile = tile = wid // net.n_col
    m = blk * tile
    per = h * tile // LANES

    def work(buf, b):
        for q in range(net.n_col):
            z = dot_t(w_ref[...], buf[q])
            z = z[:SUB, :m] + z[SUB:16, tile:tile + m] + z[16:, 2 * tile:2 * tile + m]
            for c in range(oc):
                for t in range(m // LANES):
                    mine[q, pl.ds(c * per + b * (m // LANES) + t, 1), :] = z[c:c + 1, t * LANES:(t + 1) * LANES]
    rows.run((buf0, buf1), work)
    pl.semaphore_wait(barrier, net.n_col - 1)
    copies = []
    for k, col in enumerate(cols[1:]):
        copies.append(pltpu.make_async_remote_copy(
            src_ref=mine.at[col], dst_ref=recv.at[net.col], send_sem=send_sems.at[k], recv_sem=recv_sems.at[k],
            device_id={'col': col}, device_id_type=MESH))
        copies[-1].start()
    recv[net.col] = mine[net.col]
    for copy in copies:
        copy.wait()
    i, j = iota((LANES, LANES), 0), iota((LANES, LANES), 1)
    splits = wid // BASE
    lane, run = lax.rem(j, tile), j // tile
    src = run * tile + lax.rem(lane, 2) * (tile // 2) + lax.rem(lane // 2, splits // 2) * (tile // splits) + lane // splits
    perm = (i == src).astype(F32)
    for q in range(net.n_col):
        out_ref[q] = exact_dot(recv[q], perm)


def last_conv(x, tot, norm, w, h, wid, net_shape, blk, cid):
    n_col = net_shape[1]
    ch, oc = w.shape[2:]
    wt = jnp.zeros((3, SUB, 3 * ch), BF16).at[:, :oc].set(w.reshape(3, 3 * ch, oc).transpose(0, 2, 1))
    buf = pltpu.VMEM((n_col, (blk + 2) * wid // n_col, 3 * ch), BF16)
    shape = (n_col, oc * h * wid // n_col // LANES, LANES)
    return pl.pallas_call(
        functools.partial(last_kernel, (net_shape, wid, h, blk, oc)),
        out_shape=jax.ShapeDtypeStruct(shape, F32),
        in_specs=[VMEM_SPEC] * 4, out_specs=VMEM_SPEC,
        scratch_shapes=[buf, buf, pltpu.VMEM(shape, F32), pltpu.VMEM(shape, F32)] + [pltpu.SemaphoreType.DMA((n_col,))] * 2,
        compiler_params=comm_params(cid, 28),
        name='last_conv',
    )(x, tot, norm, wt.reshape(-1, 3 * ch))


def device_body(net_shape, tokens, mod_vec, w_fc1, w_fc2, w_final, conv_in, norm_attn, w_qkv, w_proj,
                norm0_a, conv0_a, norm0_b, conv0_b, upconv_0, norm1_a, conv1_a, norm1_b, conv1_b, upconv_1,
                norm2_a, conv2_a, norm2_b, conv2_b, skip_2, upconv_2, norm3_a, conv3_a, norm3_b, conv3_b,
                skip_3, norm_out, conv_out):
    n_col = net_shape[1]
    trows, tok_w, d = tokens.shape
    full = mlp(tokens.reshape(-1, d), tok_w, mod_vec, w_fc1, w_fc2, w_final, net_shape, 1)
    h, wid = 2 * trows, 2 * tok_w
    f, tot = attention(full.reshape(-1, full.shape[-1]), conv_in, norm_attn, w_qkv, w_proj, net_shape, 2)
    u = f.reshape(-1, f.shape[-1])
    blocks = [(norm0_a, conv0_a, norm0_b, conv0_b, (), upconv_0, h, h + 2, h + 1, 15),
              (norm1_a, conv1_a, norm1_b, conv1_b, (), upconv_1, 16, 22, 13, 13),
              (norm2_a, conv2_a, norm2_b, conv2_b, (skip_2,), upconv_2, 16, 13, 10, 20),
              (norm3_a, conv3_a, norm3_b, conv3_b, (skip_3,), None, 16, 16, 0, 24)]
    cid, n = 3, net_shape[0] * n_col
    for norm_a, conv_a, norm_b, conv_b, skip, up, blk_a, blk_b, blk_up, mib in blocks:
        last = up is None
        rows = -(-(h + 2) // blk_b) * blk_b
        skip = [(m, rows // (SUB if rows % SUB == 0 else 5), rows) for m in skip]
        first = conv(u, tot, norm_a, conv_a, h, wid, n, blk_a, 0, True, 2, last, (), *skip or [()])
        name = 'level_w%d' % wid
        if last:
            g, tot, *short = launch([first], net_shape, cid, mib, name + 'a')
            g, short = g.reshape(-1, g.shape[-1]), short
        else:
            g, tot, *short = [Made(first, i) for i, _ in enumerate(first[2])]
        second = conv(g, tot, norm_b, conv_b, h, wid, n, blk_b, 1, last, 0, last, short or (u,), ())
        if last:
            f, tot = launch([second], net_shape, cid + 1, mib, name + 'b')
        else:
            third = upconv(Made(second, 0), up, h, wid, n, blk_up)
            u, tot = launch([first, second, third], net_shape, cid, mib, name)
            u = u.reshape(-1, u.shape[-1])
            h, wid = 2 * h, 2 * wid
        cid += 2
    tile = last_conv(f.reshape(-1, f.shape[-1]), tot, norm_out, conv_out, h, wid, net_shape, 16, cid)
    tile = tile.reshape(n_col, -1, h, wid // n_col).transpose(0, 2, 3, 1)
    return tile.reshape(n_col * h, wid // n_col, -1)


def solution(mesh):
    body_fn = functools.partial(device_body, (mesh.shape['row'], mesh.shape['col']))
    tok_spec = P(('batch', 'row', 'col'), None, None)
    out_spec = P(('batch', 'row'), 'col', None)
    return jax.shard_map(body_fn, mesh=mesh, in_specs=(tok_spec,) + (P(),) * 31, out_specs=out_spec, check_vma=False)
```
